32 devices in a mesh: dom: 8 (over z, y), grp: 4 (over x, core).
Axes of the slice: x: 2, y: 2, z: 4, core: 2. Of those that a mesh axis runs over, the one named last changes fastest.
Arguments:
- element_faces: int32 [4, 1024], P(None, 'dom'), may hold values from 0 to 1023, as said below
- interior_load: bfloat16 [80, 1024], P(None, 'dom'), may hold values from -6 to 6
- inverses: bfloat16 [80, 80, 1024], P('grp', None, 'dom'), may hold values from -0.625 to 0.625
- lift_operator: float32 [80, 240], P('grp'), may hold values from -0.625 to 0.625
- face_area: float32 [4, 1024], P(None, 'dom'), may hold values from 0.3 to 27
- columns: int32 [7, 1024], P(None, 'dom'), may hold values from -1 to 1023, as said below
- blocks: float32 [7, 60, 60, 1024], P(None, 'grp', None, 'dom'), may hold values from -0.00119 to 0.00119
- diagonal: float32 [60, 1024], P('grp', 'dom'), may hold values from 1.02 to 1.3
Outputs:
- solution: float32 [60, 1024], P('grp', 'dom')
- residual: float32 [60, 1024], P('grp', 'dom')
The draws below stay inside these ranges and needn't reach their ends.
Inputs may be any that keep to these rules, and one draw needn't show every extreme that they name: `element_faces`: every face block of an element is owned by the element's own index of dom or the one before or after it; an index owns the face blocks i * 128 to (i + 1) * 128 - 1. `columns`: slot 0 of a face block row holds the block itself. Every other nonnegative entry is a face block owned by the row's own index of dom or the one before or after it, and within one slot no number appears twice.
All inputs are finite; a program needn't handle non-finite values.
Results may differ from the reference program's by a relative error of at most 0.0003.
Values sent between devices are 32-bit elements; how exact they have to be, the bound alone decides.
No kernel may reach another device: no remote copies, remote signals or barrier semaphores. Data moves between devices by JAX's collectives and lax.ppermute only.
A program may use at most 64 MiB of HBM per device.

```python
import jax
import jax.numpy as jnp
from jax import lax

FB = 60
NI = 80
SLOTS = 7
ITERS = 8
F_DEV = 128
E_DEV = 128
FACES = 1024
ELEMS = 1024
N_DOM = 8


def draw_columns(key, part):
    faces = F_DEV * N_DOM
    half = F_DEV // 2
    groups = faces // half
    position = jnp.arange(faces, dtype=jnp.int32)
    listing = [position]
    for slot_index in range(1, SLOTS):
        slot_key = jax.random.fold_in(key, slot_index + 11)
        shift_key, order_key, drop_key = jax.random.split(slot_key, 3)
        offset = jax.random.randint(shift_key, (), -half, half + 1, dtype=jnp.int32)
        target = position + offset
        inside = (target >= 0) & (target < faces)
        safe_target = jnp.clip(target, 0, faces - 1)
        scores = jax.random.randint(order_key, (groups, half), 0, 1 << 20, dtype=jnp.int32) * half + jnp.arange(half, dtype=jnp.int32)[None, :]
        shuffle = jnp.argsort(scores, axis=1).astype(jnp.int32)
        moved = safe_target // half * half + shuffle[safe_target // half, safe_target % half]
        kept = jax.random.randint(drop_key, (faces,), 0, 8, dtype=jnp.int32) > 0
        listing.append(jnp.where(inside & kept, moved, -1))
    return jnp.stack(listing).astype(jnp.int32)


def draw_element_faces(key, part):
    elements = E_DEV * N_DOM
    owner = jnp.arange(elements, dtype=jnp.int32) // E_DEV
    lowest = jnp.maximum(owner - 1, 0) * F_DEV
    highest = jnp.minimum(owner + 2, N_DOM) * F_DEV
    drawn = jax.random.randint(jax.random.fold_in(key, 5), (4, elements), lowest[None, :], highest[None, :], dtype=jnp.int32)
    return drawn.astype(jnp.int32)


def draw_face_area(key, part):
    elements = E_DEV * N_DOM
    ramp = 1.0 + 2.0 * jnp.arange(elements, dtype=jnp.float32) / elements
    exponent = jax.random.uniform(jax.random.fold_in(key, 7), (4, elements), jnp.float32, jnp.log(0.3), jnp.log(3.0))
    return (jnp.exp(exponent) * ramp[None, :]).astype(jnp.float32)


def draw_blocks(key, part):
    faces = F_DEV * N_DOM
    edge = 0.00119
    shape = (SLOTS, FB, FB, faces)
    block_key = jax.random.fold_in(key, 21)
    values = jax.random.uniform(block_key, shape, jnp.float32, -edge, edge)
    return values.astype(jnp.float32)


def levels(rng, extent, shards, smallest, largest):
    def one(dim, parts):
        steps = jax.random.uniform(jax.random.fold_in(jax.random.fold_in(rng, 6), dim), (parts,), jnp.float32, smallest / len(shards), largest / len(shards))
        return jnp.repeat(jnp.exp(steps), extent[dim] // parts).reshape((-1,) + (1,) * (len(extent) - dim - 1))

    factor_of = one(*shards[0])
    for cut in shards[1:]:
        factor_of = factor_of * one(*cut)
    return factor_of


def centred(stream_key, extent, width, bound, cuts=(), kind=jnp.bfloat16):
    factor_of = levels(stream_key, extent, cuts, -0.22, 0.18) if cuts else 1.0
    values = jax.random.normal(stream_key, extent, jnp.float32) * width * factor_of
    return jnp.minimum(jnp.maximum(values, -bound), bound).astype(kind)


def setup_inputs(seed: int = 0) -> dict:
    key_list = jax.random.split(jax.random.key(seed), 9)
    return {
        "element_faces": draw_element_faces(jax.random.fold_in(key_list[8], 71), 0),
        "interior_load": centred(key_list[1], (NI, ELEMS), 1.0, 6.0, ((1, 8),)),
        "inverses": centred(key_list[2], (NI, NI, ELEMS), NI ** -0.5, 0.625, ((0, 4), (2, 8))),
        "lift_operator": centred(key_list[3], (NI, 4 * FB), NI ** -0.5, 0.625, ((0, 4),), jnp.float32),
        "face_area": draw_face_area(jax.random.fold_in(key_list[8], 71), 0),
        "columns": draw_columns(jax.random.fold_in(key_list[8], 71), 0),
        "blocks": draw_blocks(jax.random.fold_in(key_list[8], 71), 0),
        "diagonal": jnp.clip(1.02 + 0.27999997 * jax.random.uniform(key_list[7], (FB, FACES), jnp.float32) ** levels(key_list[7], (FB, FACES), ((0, 4), (1, 8)), -0.2, 0.2), 1.02, 1.3),
    }


def operate(field, blocks, columns, diagonal):
    usable = columns >= 0
    index = jnp.where(usable, columns, 0).astype(jnp.int32)
    result = diagonal * field
    for slot_index in range(SLOTS):
        matrix = blocks[slot_index]
        picked = jnp.where(usable[slot_index][None, :], field[:, index[slot_index]], jnp.zeros((), field.dtype))
        result = result + jnp.einsum("ijf,jf->if", matrix, picked, precision=lax.Precision.HIGHEST)
        transposed = jnp.einsum("ijf,if->jf", matrix, field, precision=lax.Precision.HIGHEST)
        transposed = jnp.where(usable[slot_index][None, :], transposed, jnp.zeros((), field.dtype))
        result = result + jax.ops.segment_sum(transposed.T, index[slot_index], num_segments=FACES).T
    return result


def reference(element_faces, interior_load, inverses, lift_operator, face_area, columns, blocks, diagonal):
    interior = jnp.einsum("ije,je->ie", inverses.astype(jnp.float32), interior_load.astype(jnp.float32), precision=lax.Precision.HIGHEST)
    lifted = jnp.dot(lift_operator.T, interior, precision=lax.Precision.HIGHEST)
    contribution = -(lifted.reshape(4, FB, ELEMS) * face_area[:, None, :])
    entries = jnp.transpose(contribution, (0, 2, 1)).reshape(4 * ELEMS, FB)
    right_side = jax.ops.segment_sum(entries, element_faces.reshape(-1).astype(jnp.int32), num_segments=FACES).T
    solution = jnp.zeros_like(right_side)
    residual = right_side
    direction = right_side
    norm_now = jnp.sum(residual * residual)
    for iteration in range(ITERS):
        image = operate(direction, blocks, columns, diagonal)
        alpha = norm_now / jnp.sum(direction * image)
        solution = solution + alpha * direction
        residual = residual - alpha * image
        norm_next = jnp.sum(residual * residual)
        direction = residual + (norm_next / norm_now) * direction
        norm_now = norm_next
    return solution, residual
```

```python
import functools

import jax
import jax.numpy as jnp
from jax import lax
from jax.experimental import pallas as pl
from jax.experimental.pallas import tpu as pltpu
from jax.sharding import PartitionSpec as P

ITERS = 8
SUB = 8
ALL = ("dom", "grp")


def up(n, m):
    return (n + m - 1) // m * m


def parts3(x):
    hi = x.astype(jnp.bfloat16)
    rest = x - hi.astype(jnp.float32)
    mid = rest.astype(jnp.bfloat16)
    low = (rest - mid.astype(jnp.float32)).astype(jnp.bfloat16)
    return jnp.concatenate([hi, mid, low], axis=0)


def sum3(y):
    n = y.shape[0] // 3
    return y[:n] + y[n : 2 * n] + y[2 * n :]


def near(step, n_dom):
    return lax.rem(lax.axis_index("dom") + n_dom - 1 + step, n_dom)


def post(out_ref, slab_ref, n_dom, n_grp, width, faces):
    for t in range(3):
        base = near(t, n_dom) * n_grp
        for q in range(n_grp):
            rows = slab_ref[q * width : (q + 1) * width, t * faces : (t + 1) * faces]
            out_ref[base + q, :width, :] = rows


def owned(recv_ref, n_dom, n_grp, width):
    total = None
    for t in range(3):
        base = near(t, n_dom) * n_grp
        for q in range(n_grp):
            piece = recv_ref[base + q, :width, :]
            total = piece if total is None else total + piece
    return total


def rhs_kernel(n_dom, n_grp, width, inv_ref, load_ref, lift_ref, area_ref, hot_ref, out_ref, slab_ref):
    faces = out_ref.shape[2]
    full = width * n_grp
    load = load_ref[...].astype(jnp.float32)
    rows = [
        jnp.sum(inv_ref[i].astype(jnp.float32) * load, axis=0, keepdims=True)
        for i in range(inv_ref.shape[0])
    ]
    u = jnp.concatenate(rows, axis=0)
    lifted = lax.dot_general(
        lift_ref[...], u, (((0,), (0,)), ((), ())),
        precision=lax.Precision.HIGHEST, preferred_element_type=jnp.float32,
    )
    pad = up(full, 16) - full
    total = None
    for k in range(area_ref.shape[0]):
        entry = -lifted[k * full : (k + 1) * full] * area_ref[k : k + 1, :]
        entry = jnp.concatenate([entry, jnp.zeros((pad, entry.shape[1]), jnp.float32)], axis=0)
        e = entry.shape[1]
        part = jnp.dot(parts3(entry), hot_ref[k * e : (k + 1) * e, :], preferred_element_type=jnp.float32)
        total = part if total is None else total + part
    slab_ref[...] = sum3(total)
    post(out_ref, slab_ref, n_dom, n_grp, width, faces)


def apply_kernel(n_dom, n_grp, recv_ref, r_ref, diag_ref, blocks_ref, hot_ref, back_ref, out_ref, near_ref, slab_ref, pick_ref, turn_ref):
    slots, width, full, faces = blocks_ref.shape
    tall = up(full, 16)
    for t in range(3):
        base = near(t, n_dom) * n_grp
        for q in range(n_grp):
            slab_ref[q * width : (q + 1) * width, t * faces : (t + 1) * faces] = recv_ref[base + q, :width, :]
    slab_ref[full:tall, :] = jnp.zeros((tall - full, 3 * faces), jnp.float32)
    pick_ref[...] = sum3(jnp.dot(parts3(slab_ref[...]), hot_ref[...], preferred_element_type=jnp.float32))
    wide = [jnp.broadcast_to(r_ref[a : a + 1, :], (SUB, faces)) for a in range(width)]
    turn_ref[full:tall, :] = jnp.zeros((tall - full, slots * faces), jnp.float32)
    total = [None] * width
    for low in range(0, full, SUB):
        high = min(low + SUB, full)
        acc = [None] * width
        for s in range(slots):
            cols = slice(s * faces, (s + 1) * faces)
            picked = pick_ref[low:high, cols]
            turned = None
            for a in range(width):
                tile = blocks_ref[s, a, low:high, :]
                forward = tile * picked
                backward = tile * wide[a][: high - low]
                acc[a] = forward if acc[a] is None else acc[a] + forward
                turned = backward if turned is None else turned + backward
            turn_ref[low:high, cols] = turned
        for a in range(width):
            line = jnp.sum(acc[a], axis=0, keepdims=True)
            total[a] = line if total[a] is None else total[a] + line
    forward = jnp.concatenate(total, axis=0)
    slab_ref[...] = sum3(jnp.dot(parts3(turn_ref[...]), back_ref[...], preferred_element_type=jnp.float32))
    post(out_ref, slab_ref, n_dom, n_grp, width, faces)
    r = r_ref[...]
    plain = diag_ref[...] * r + forward
    near_ref[...] = plain
    square = jnp.sum(r * r, axis=0, keepdims=True)
    cross = jnp.sum(r * (plain + forward), axis=0, keepdims=True)
    lane = lax.broadcasted_iota(jnp.int32, (1, faces), 1)
    half = faces // 2
    line = jnp.where(lane < half, square + pltpu.roll(square, half, 1), cross + pltpu.roll(cross, half, 1))
    for n in range(n_dom * n_grp):
        out_ref[n, width : width + 1, :] = line


def start_kernel(n_dom, n_grp, recv_ref, out_ref, r_ref):
    width = r_ref.shape[0]
    r = owned(recv_ref, n_dom, n_grp, width)
    r_ref[...] = r
    for n in range(n_dom * n_grp):
        out_ref[n, :width, :] = r


def update_kernel(n_dom, n_grp, first, last, *refs):
    refs = list(refs)
    recv_ref, near_ref, r_ref = refs[:3]
    del refs[:3]
    if not first:
        s_ref, p_ref, x_ref, scal_ref = refs[:4]
        del refs[:4]
    width, faces = r_ref.shape
    lines = jnp.sum(recv_ref[:, width, :], axis=0, keepdims=True)
    lane = lax.broadcasted_iota(jnp.int32, (1, faces), 1)
    low = lane < faces // 2
    norm = jnp.sum(jnp.where(low, lines, 0.0), axis=1, keepdims=True)
    cross = jnp.sum(jnp.where(low, 0.0, lines), axis=1, keepdims=True)
    w = near_ref[...] + owned(recv_ref, n_dom, n_grp, width)
    r = r_ref[...]
    if first:
        alpha = norm / cross
        s, p = w, r
        x = alpha * p
    else:
        beta = norm / scal_ref[0:1, 0:1]
        alpha = norm / (cross - beta * norm / scal_ref[1:2, 0:1])
        s = w + beta * s_ref[...]
        p = r + beta * p_ref[...]
        x = x_ref[...] + alpha * p
    r = r - alpha * s
    if last:
        xo_ref, ro_ref = refs
        xo_ref[...] = x
        ro_ref[...] = r
        return
    out_ref, ro_ref, so_ref, po_ref, xo_ref, scalo_ref = refs
    for n in range(n_dom * n_grp):
        out_ref[n, :width, :] = r
    ro_ref[...] = r
    so_ref[...] = s
    po_ref[...] = p
    xo_ref[...] = x
    scalo_ref[0:1, :] = jnp.broadcast_to(norm, (1, faces))
    scalo_ref[1:2, :] = jnp.broadcast_to(alpha, (1, faces))


def call(kernel, outs, args, scratch=(), name=None):
    vmem = pl.BlockSpec(memory_space=pltpu.VMEM)
    return pl.pallas_call(
        kernel,
        out_shape=outs,
        in_specs=[vmem] * len(args),
        out_specs=jax.tree.map(lambda _: vmem, outs),
        scratch_shapes=list(scratch),
        name=name,
    )(*args)


def on_device(
    element_faces, interior_load, inverses, lift_operator, face_area, columns, blocks, diagonal
):
    n_dom, n_grp = lax.axis_size("dom"), lax.axis_size("grp")
    slots, width, full, faces = blocks.shape
    tall = up(full, 16)
    pieces = jax.ShapeDtypeStruct((n_dom * n_grp, up(width + 1, SUB), faces), jnp.float32)
    field = jax.ShapeDtypeStruct((width, faces), jnp.float32)
    f32 = jnp.float32

    low_face = (lax.axis_index("dom") - 1) * faces
    window = jnp.arange(3 * faces, dtype=jnp.int32)
    here = jnp.where(columns >= 0, columns - low_face, -1).reshape(-1)
    hot = (window[:, None] == here[None, :]).astype(jnp.bfloat16)
    back = (here[:, None] == window[None, :]).astype(jnp.bfloat16)
    owner = (element_faces - low_face).reshape(-1)
    gathered = (owner[:, None] == window[None, :]).astype(jnp.bfloat16)

    def exchange(v):
        return lax.all_to_all(v, ALL, 0, 0)

    slab = pltpu.VMEM((tall, 3 * faces), f32)
    sent = call(
        functools.partial(rhs_kernel, n_dom, n_grp, width),
        pieces,
        (inverses, interior_load, lift_operator, face_area, gathered),
        [slab],
        name="rhs",
    )
    sent, r = call(
        functools.partial(start_kernel, n_dom, n_grp), (pieces, field), (exchange(sent),), name="start"
    )
    state = ()
    for iteration in range(ITERS):
        sent, plain = call(
            functools.partial(apply_kernel, n_dom, n_grp),
            (pieces, field),
            (exchange(sent), r, diagonal, blocks, hot, back),
            [slab, pltpu.VMEM((tall, slots * faces), f32), pltpu.VMEM((tall, slots * faces), f32)],
            name="apply",
        )
        first, last = iteration == 0, iteration + 1 == ITERS
        outs = (field, field) if last else (pieces, field, field, field, field, jax.ShapeDtypeStruct((2, faces), f32))
        got = call(
            functools.partial(update_kernel, n_dom, n_grp, first, last),
            outs,
            (exchange(sent), plain, r) + state,
            name="update",
        )
        if last:
            return got
        sent, r, *state = got
        state = tuple(state)


def solution(mesh):
    placed = (
        P(None, "dom"),
        P(None, "dom"),
        P("grp", None, "dom"),
        P("grp", None),
        P(None, "dom"),
        P(None, "dom"),
        P(None, "grp", None, "dom"),
        P("grp", "dom"),
    )
    return jax.shard_map(
        on_device,
        mesh=mesh,
        in_specs=placed,
        out_specs=(P("grp", "dom"), P("grp", "dom")),
        check_vma=False,
    )
```

```python
import functools

import jax
import jax.numpy as jnp
from jax import lax
from jax.experimental import pallas as pl
from jax.experimental.pallas import tpu as pltpu
from jax.sharding import PartitionSpec as P

ITERS = 8
SUB = 8
VMEM_GRANT = 16 * 1024 * 1024
ALL = ("dom", "grp")


def up(n, m):
    return (n + m - 1) // m * m


def parts3(x):
    hi = x.astype(jnp.bfloat16)
    rest = x - hi.astype(jnp.float32)
    mid = rest.astype(jnp.bfloat16)
    low = (rest - mid.astype(jnp.float32)).astype(jnp.bfloat16)
    return jnp.concatenate([hi, mid, low], axis=0)


def sum3(y):
    n = y.shape[0] // 3
    return y[:n] + y[n : 2 * n] + y[2 * n :]


def near(step, n_dom):
    return lax.rem(lax.axis_index("dom") + n_dom - 1 + step, n_dom)


def post(out_ref, slab_ref, n_dom, n_grp, width, faces):
    for t in range(3):
        base = near(t, n_dom) * n_grp
        for q in range(n_grp):
            rows = slab_ref[q * width : (q + 1) * width, t * faces : (t + 1) * faces]
            out_ref[base + q, :width, :] = rows


def owned(recv_ref, n_dom, n_grp, width):
    total = None
    for t in range(3):
        base = near(t, n_dom) * n_grp
        for q in range(n_grp):
            piece = recv_ref[base + q, :width, :]
            total = piece if total is None else total + piece
    return total


def rhs_kernel(n_dom, n_grp, width, cols_ref, owner_ref, inv_ref, load_ref, lift_ref, area_ref, out_ref, hot_ref, back_ref, slab_ref):
    faces = out_ref.shape[2]
    full = width * n_grp
    slots, sides = cols_ref.shape[0], owner_ref.shape[0]
    low_face = (lax.axis_index("dom") - 1) * faces
    cols = cols_ref[...]
    here = jnp.where(cols >= 0, cols - low_face, -1)
    place = lax.broadcasted_iota(jnp.int32, (3 * faces, faces), 0)
    for s in range(slots):
        hit = place == here[s : s + 1, :]
        hot_ref[:, s * faces : (s + 1) * faces] = jnp.where(hit, 1.0, 0.0).astype(jnp.bfloat16)
    lists = jnp.concatenate([here, owner_ref[...] - low_face], axis=0)
    tall = up(slots + sides, SUB)
    blank = jnp.full((tall - slots - sides, faces), -1, jnp.int32)
    flipped = jnp.concatenate([lists, blank], axis=0).astype(jnp.float32).T
    window = lax.broadcasted_iota(jnp.int32, (faces, 3 * faces), 1).astype(jnp.float32)

    def scatter_of(n):
        return jnp.where(window == flipped[:, n : n + 1], 1.0, 0.0).astype(jnp.bfloat16)

    for s in range(slots):
        back_ref[s * faces : (s + 1) * faces, :] = scatter_of(s)
    load = load_ref[...].astype(jnp.float32)
    rows = [
        jnp.sum(inv_ref[i].astype(jnp.float32) * load, axis=0, keepdims=True)
        for i in range(inv_ref.shape[0])
    ]
    u = jnp.concatenate(rows, axis=0)
    lifted = lax.dot_general(
        lift_ref[...], u, (((0,), (0,)), ((), ())),
        precision=lax.Precision.HIGHEST, preferred_element_type=jnp.float32,
    )
    pad = up(full, 16) - full
    total = None
    for k in range(sides):
        entry = -lifted[k * full : (k + 1) * full] * area_ref[k : k + 1, :]
        entry = jnp.concatenate([entry, jnp.zeros((pad, entry.shape[1]), jnp.float32)], axis=0)
        part = jnp.dot(parts3(entry), scatter_of(slots + k), preferred_element_type=jnp.float32)
        total = part if total is None else total + part
    slab_ref[...] = sum3(total)
    post(out_ref, slab_ref, n_dom, n_grp, width, faces)


def apply_kernel(n_dom, n_grp, recv_ref, r_ref, diag_ref, blocks_ref, hot_ref, back_ref, out_ref, near_ref, slab_ref, pick_ref, turn_ref):
    slots, width, full, faces = blocks_ref.shape
    tall = up(full, 16)
    for t in range(3):
        base = near(t, n_dom) * n_grp
        for q in range(n_grp):
            slab_ref[q * width : (q + 1) * width, t * faces : (t + 1) * faces] = recv_ref[base + q, :width, :]
    slab_ref[full:tall, :] = jnp.zeros((tall - full, 3 * faces), jnp.float32)
    pick_ref[...] = sum3(jnp.dot(parts3(slab_ref[...]), hot_ref[...], preferred_element_type=jnp.float32))
    wide = [jnp.broadcast_to(r_ref[a : a + 1, :], (SUB, faces)) for a in range(width)]
    turn_ref[full:tall, :] = jnp.zeros((tall - full, slots * faces), jnp.float32)
    total = [None] * width
    for low in range(0, full, SUB):
        high = min(low + SUB, full)
        acc = [None] * width
        for s in range(slots):
            cols = slice(s * faces, (s + 1) * faces)
            picked = pick_ref[low:high, cols]
            turned = None
            for a in range(width):
                tile = blocks_ref[s, a, low:high, :]
                forward = tile * picked
                backward = tile * wide[a][: high - low]
                acc[a] = forward if acc[a] is None else acc[a] + forward
                turned = backward if turned is None else turned + backward
            turn_ref[low:high, cols] = turned
        for a in range(width):
            line = jnp.sum(acc[a], axis=0, keepdims=True)
            total[a] = line if total[a] is None else total[a] + line
    forward = jnp.concatenate(total, axis=0)
    slab_ref[...] = sum3(jnp.dot(parts3(turn_ref[...]), back_ref[...], preferred_element_type=jnp.float32))
    post(out_ref, slab_ref, n_dom, n_grp, width, faces)
    r = r_ref[...]
    plain = diag_ref[...] * r + forward
    near_ref[...] = plain
    square = jnp.sum(r * r, axis=0, keepdims=True)
    cross = jnp.sum(r * (plain + forward), axis=0, keepdims=True)
    lane = lax.broadcasted_iota(jnp.int32, (1, faces), 1)
    half = faces // 2
    line = jnp.where(lane < half, square + pltpu.roll(square, half, 1), cross + pltpu.roll(cross, half, 1))
    for n in range(n_dom * n_grp):
        out_ref[n, width : width + 1, :] = line


def start_kernel(n_dom, n_grp, recv_ref, out_ref, r_ref):
    width = r_ref.shape[0]
    r = owned(recv_ref, n_dom, n_grp, width)
    r_ref[...] = r
    for n in range(n_dom * n_grp):
        out_ref[n, :width, :] = r


def update_kernel(n_dom, n_grp, first, last, *refs):
    refs = list(refs)
    recv_ref, near_ref, r_ref = refs[:3]
    del refs[:3]
    if not first:
        s_ref, p_ref, x_ref, scal_ref = refs[:4]
        del refs[:4]
    width, faces = r_ref.shape
    lines = jnp.sum(recv_ref[:, width, :], axis=0, keepdims=True)
    lane = lax.broadcasted_iota(jnp.int32, (1, faces), 1)
    low = lane < faces // 2
    norm = jnp.sum(jnp.where(low, lines, 0.0), axis=1, keepdims=True)
    cross = jnp.sum(jnp.where(low, 0.0, lines), axis=1, keepdims=True)
    w = near_ref[...] + owned(recv_ref, n_dom, n_grp, width)
    r = r_ref[...]
    if first:
        alpha = norm / cross
        s, p = w, r
        x = alpha * p
    else:
        beta = norm / scal_ref[0:1, 0:1]
        alpha = norm / (cross - beta * norm / scal_ref[1:2, 0:1])
        s = w + beta * s_ref[...]
        p = r + beta * p_ref[...]
        x = x_ref[...] + alpha * p
    r = r - alpha * s
    if last:
        xo_ref, ro_ref = refs
        xo_ref[...] = x
        ro_ref[...] = r
        return
    out_ref, ro_ref, so_ref, po_ref, xo_ref, scalo_ref = refs
    for n in range(n_dom * n_grp):
        out_ref[n, :width, :] = r
    ro_ref[...] = r
    so_ref[...] = s
    po_ref[...] = p
    xo_ref[...] = x
    scalo_ref[0:1, :] = jnp.broadcast_to(norm, (1, faces))
    scalo_ref[1:2, :] = jnp.broadcast_to(alpha, (1, faces))


def call(kernel, outs, args, scratch=(), name=None):
    vmem = pl.BlockSpec(memory_space=pltpu.VMEM)
    return pl.pallas_call(
        kernel,
        out_shape=outs,
        in_specs=[vmem] * len(args),
        out_specs=jax.tree.map(lambda _: vmem, outs),
        scratch_shapes=list(scratch),
        name=name,
        compiler_params=pltpu.CompilerParams(vmem_limit_bytes=VMEM_GRANT),
    )(*args)


def on_device(
    element_faces, interior_load, inverses, lift_operator, face_area, columns, blocks, diagonal
):
    n_dom, n_grp = lax.axis_size("dom"), lax.axis_size("grp")
    slots, width, full, faces = blocks.shape
    tall = up(full, 16)
    pieces = jax.ShapeDtypeStruct((n_dom * n_grp, up(width + 1, SUB), faces), jnp.float32)
    field = jax.ShapeDtypeStruct((width, faces), jnp.float32)
    f32 = jnp.float32

    def exchange(v):
        return lax.all_to_all(v, ALL, 0, 0)

    slab = pltpu.VMEM((tall, 3 * faces), f32)
    sent, hot, back = call(
        functools.partial(rhs_kernel, n_dom, n_grp, width),
        (
            pieces,
            jax.ShapeDtypeStruct((3 * faces, slots * faces), jnp.bfloat16),
            jax.ShapeDtypeStruct((slots * faces, 3 * faces), jnp.bfloat16),
        ),
        (columns, element_faces, inverses, interior_load, lift_operator, face_area),
        [slab],
        name="rhs",
    )
    sent, r = call(
        functools.partial(start_kernel, n_dom, n_grp), (pieces, field), (exchange(sent),), name="start"
    )
    state = ()
    for iteration in range(ITERS):
        sent, plain = call(
            functools.partial(apply_kernel, n_dom, n_grp),
            (pieces, field),
            (exchange(sent), r, diagonal, blocks, hot, back),
            [slab, pltpu.VMEM((tall, slots * faces), f32), pltpu.VMEM((tall, slots * faces), f32)],
            name="apply",
        )
        first, last = iteration == 0, iteration + 1 == ITERS
        outs = (field, field) if last else (pieces, field, field, field, field, jax.ShapeDtypeStruct((2, faces), f32))
        got = call(
            functools.partial(update_kernel, n_dom, n_grp, first, last),
            outs,
            (exchange(sent), plain, r) + state,
            name="update",
        )
        if last:
            return got
        sent, r, *state = got
        state = tuple(state)


def solution(mesh):
    placed = (
        P(None, "dom"),
        P(None, "dom"),
        P("grp", None, "dom"),
        P("grp", None),
        P(None, "dom"),
        P(None, "dom"),
        P(None, "grp", None, "dom"),
        P("grp", "dom"),
    )
    return jax.shard_map(
        on_device,
        mesh=mesh,
        in_specs=placed,
        out_specs=(P("grp", "dom"), P("grp", "dom")),
        check_vma=False,
    )
```

```python
import functools

import jax
import jax.numpy as jnp
from jax import lax
from jax.experimental import pallas as pl
from jax.experimental.pallas import tpu as pltpu
from jax.sharding import PartitionSpec as P

ITERS = 8
SUB = 8
ALL = ("dom", "grp")
VMEM_GRANT = 16 * 1024 * 1024


def up(n, m):
    return (n + m - 1) // m * m


def parts3(x):
    hi = x.astype(jnp.bfloat16)
    rest = x - hi.astype(jnp.float32)
    mid = rest.astype(jnp.bfloat16)
    low = (rest - mid.astype(jnp.float32)).astype(jnp.bfloat16)
    return jnp.concatenate([hi, mid, low], axis=0)


def sum3(y):
    n = y.shape[0] // 3
    return y[:n] + y[n : 2 * n] + y[2 * n :]


class Plan:
    def __init__(self, width, faces):
        self.n_dom, self.n_grp = lax.axis_size("dom"), lax.axis_size("grp")
        self.width, self.faces = width, faces
        self.half = width // 2
        self.rows = self.half + 1
        self.tall = up(self.rows, SUB)

    def base(self, shift, lower):
        shift += self.n_dom // 2 if lower else 0
        return lax.rem(lax.axis_index("dom") + (shift + self.n_dom), self.n_dom) * self.n_grp

    def kept(self, shift):
        return self.base(shift - self.n_dom // 2, False)

    def left(self):
        return lax.broadcasted_iota(jnp.int32, (1, self.faces), 1) < self.faces // 2

    def split(self, rows, line):
        h, left = self.half, self.left()
        middle = rows[h : h + 1]
        upper = jnp.where(left, middle, line)
        lower = jnp.where(left, pltpu.roll(middle, self.faces // 2, 1), line)
        return (
            jnp.concatenate([rows[:h], upper], axis=0),
            jnp.concatenate([rows[h + 1 :], lower], axis=0),
        )

    def join(self, upper, lower):
        h = self.half
        middle = jnp.where(self.left(), upper[h : h + 1], pltpu.roll(lower[h : h + 1], self.faces // 2, 1))
        return jnp.concatenate([upper[:h], middle, lower[:h]], axis=0)

    def post(self, out_ref, slab_ref, line):
        w, f = self.width, self.faces
        for t in range(3):
            for q in range(self.n_grp):
                rows = slab_ref[q * w : (q + 1) * w, t * f : (t + 1) * f]
                for lower, piece in enumerate(self.split(rows, line)):
                    out_ref[self.base(t - 1, lower) + q, : self.rows, :] = piece

    def owned(self, recv_ref):
        sums = []
        for first in (functools.partial(self.base, lower=False), self.kept):
            total = None
            for t in range(3):
                for q in range(self.n_grp):
                    piece = recv_ref[first(t - 1) + q, : self.rows, :]
                    total = piece if total is None else total + piece
            row = lax.broadcasted_iota(jnp.int32, (self.rows, self.faces), 0)
            lane = lax.broadcasted_iota(jnp.int32, (self.rows, self.faces), 1)
            sums.append(jnp.where((row < self.half) | (lane < self.faces // 2), total, 0.0))
        return sums

    def spread(self, out_ref, halves):
        for first, piece in zip((functools.partial(self.base, lower=False), self.kept), halves):
            for t in range(3):
                for q in range(self.n_grp):
                    out_ref[first(t - 1) + q, : self.rows, :] = piece


def rhs_kernel(width, cols_hbm, owner_hbm, inv_hbm, load_hbm, lift_hbm, area_hbm, diag_hbm, blocks_hbm, out_ref, hot_ref, back_ref, diag_ref, blocks_ref, cols_ref, owner_ref, inv_ref, load_ref, lift_ref, area_ref, slab_ref, sems):
    fetches = [
        pltpu.make_async_copy(src, dst, sems.at[n])
        for n, (src, dst) in enumerate(
            (
                (cols_hbm, cols_ref), (owner_hbm, owner_ref), (load_hbm, load_ref), (inv_hbm, inv_ref),
                (lift_hbm, lift_ref), (area_hbm, area_ref), (diag_hbm, diag_ref), (blocks_hbm, blocks_ref),
            )
        )
    ]
    for fetch in fetches:
        fetch.start()
    faces = out_ref.shape[2]
    plan = Plan(width, faces)
    full = width * plan.n_grp
    slots, sides = cols_ref.shape[0], owner_ref.shape[0]
    low_face = (lax.axis_index("dom") - 1) * faces
    for fetch in fetches[:2]:
        fetch.wait()
    cols = cols_ref[...]
    here = jnp.where(cols >= 0, cols - low_face, -1)
    place = lax.broadcasted_iota(jnp.int32, (3 * faces, faces), 0)
    for s in range(slots):
        hit = place == here[s : s + 1, :]
        hot_ref[:, s * faces : (s + 1) * faces] = jnp.where(hit, 1.0, 0.0).astype(jnp.bfloat16)
    lists = jnp.concatenate([here, owner_ref[...] - low_face], axis=0)
    tall = up(slots + sides, SUB)
    blank = jnp.full((tall - slots - sides, faces), -1, jnp.int32)
    flipped = jnp.concatenate([lists, blank], axis=0).astype(jnp.float32).T
    window = lax.broadcasted_iota(jnp.int32, (faces, 3 * faces), 1).astype(jnp.float32)

    def scatter_of(n):
        return jnp.where(window == flipped[:, n : n + 1], 1.0, 0.0).astype(jnp.bfloat16)

    for s in range(slots):
        back_ref[s * faces : (s + 1) * faces, :] = scatter_of(s)
    for fetch in fetches[2:6]:
        fetch.wait()
    load = load_ref[...].astype(jnp.float32)
    rows = [
        jnp.sum(inv_ref[i].astype(jnp.float32) * load, axis=0, keepdims=True)
        for i in range(inv_ref.shape[0])
    ]
    u = jnp.concatenate(rows, axis=0)
    lifted = lax.dot_general(
        lift_ref[...], u, (((0,), (0,)), ((), ())),
        precision=lax.Precision.HIGHEST, preferred_element_type=jnp.float32,
    )
    pad = up(full, 16) - full
    total = None
    for k in range(sides):
        entry = -lifted[k * full : (k + 1) * full] * area_ref[k : k + 1, :]
        entry = jnp.concatenate([entry, jnp.zeros((pad, entry.shape[1]), jnp.float32)], axis=0)
        part = jnp.dot(parts3(entry), scatter_of(slots + k), preferred_element_type=jnp.float32)
        total = part if total is None else total + part
    slab_ref[...] = sum3(total)
    plan.post(out_ref, slab_ref, jnp.zeros((1, faces), jnp.float32))
    for fetch in fetches[6:]:
        fetch.wait()


def start_kernel(width, recv_ref, out_ref, r_ref):
    plan = Plan(width, recv_ref.shape[2])
    halves = plan.owned(recv_ref)
    plan.spread(out_ref, halves)
    r_ref[...] = jnp.stack(halves)


def apply_kernel(last, recv_ref, diag_ref, blocks_ref, hot_ref, back_ref, out_ref, own_ref, slab_ref, pick_ref, turn_ref):
    slots, width, full, faces = blocks_ref.shape
    plan = Plan(width, faces)
    n_dom, n_grp = plan.n_dom, plan.n_grp
    tall = slab_ref.shape[0]
    for t in range(3):
        for q in range(n_grp):
            rows = plan.join(*(recv_ref[plan.base(t - 1, lower) + q, : plan.rows, :] for lower in (False, True)))
            slab_ref[q * width : (q + 1) * width, t * faces : (t + 1) * faces] = rows
    me = lax.axis_index("grp")
    r = plan.join(*(recv_ref[plan.base(0, lower) + me, : plan.rows, :] for lower in (False, True)))
    own_ref[...] = r
    slab_ref[full:tall, :] = jnp.zeros((tall - full, 3 * faces), jnp.float32)
    pick_ref[...] = sum3(jnp.dot(parts3(slab_ref[...]), hot_ref[...], preferred_element_type=jnp.float32))
    wide = [jnp.broadcast_to(r[a : a + 1, :], (SUB, faces)) for a in range(width)]
    turn_ref[full:tall, :] = jnp.zeros((tall - full, slots * faces), jnp.float32)
    total = [None] * width
    for low in range(0, full, SUB):
        high = min(low + SUB, full)
        acc = [None] * width
        for s in range(slots):
            cols = slice(s * faces, (s + 1) * faces)
            picked = pick_ref[low:high, cols]
            turned = None
            for a in range(width):
                tile = blocks_ref[s, a, low:high, :]
                forward = tile * picked
                backward = tile * wide[a][: high - low]
                acc[a] = forward if acc[a] is None else acc[a] + forward
                turned = backward if turned is None else turned + backward
            turn_ref[low:high, cols] = turned
        for a in range(width):
            line = jnp.sum(acc[a], axis=0, keepdims=True)
            total[a] = line if total[a] is None else total[a] + line
    forward = jnp.concatenate(total, axis=0)
    plain = diag_ref[...] * r + forward
    square = jnp.sum(r * r, axis=0, keepdims=True)
    cross = jnp.sum(r * (plain + forward), axis=0, keepdims=True)
    fold = []
    for line in (square, cross):
        line = line + pltpu.roll(line, faces // 2, 1)
        fold.append(line + pltpu.roll(line, faces // 4, 1))
    lane = lax.broadcasted_iota(jnp.int32, (1, faces), 1)
    line = jnp.where(lane < faces // 4 * 3, fold[0], fold[1])
    slab_ref[...] = sum3(jnp.dot(parts3(turn_ref[...]), back_ref[...], preferred_element_type=jnp.float32))
    if last:
        for n in range(n_dom * n_grp):
            out_ref[n, width : width + 1, :] = line
        for t in range(3):
            for q in range(n_grp):
                rows = slab_ref[q * width : (q + 1) * width, t * faces : (t + 1) * faces]
                out_ref[plan.base(t - 1, False) + q, :width, :] = rows
        mine = plan.base(0, False) + me
        out_ref[mine, :width, :] = out_ref[mine, :width, :] + plain
        return
    for n in range(n_dom * n_grp):
        out_ref[n, plan.half : plan.rows, :] = line
    plan.post(out_ref, slab_ref, line)
    for lower, piece in enumerate(plan.split(plain, jnp.zeros((1, faces), jnp.float32))):
        mine = plan.base(0, lower) + me
        out_ref[mine, : plan.rows, :] = out_ref[mine, : plan.rows, :] + piece


def scalars(lines, faces, scal_ref):
    lines = jnp.sum(lines, axis=0, keepdims=True)
    lane = lax.broadcasted_iota(jnp.int32, (1, faces), 1)
    norm_at = (lane >= faces // 2) & (lane < faces // 4 * 3)
    norm = jnp.sum(jnp.where(norm_at, lines, 0.0), axis=1, keepdims=True)
    cross = jnp.sum(jnp.where(lane >= faces // 4 * 3, lines, 0.0), axis=1, keepdims=True)
    if scal_ref is None:
        return norm, norm / cross, None
    beta = norm / scal_ref[0:1, 0:1]
    return norm, norm / (cross - beta * norm / scal_ref[1:2, 0:1]), beta


def update_kernel(first, width, *refs):
    recv_ref, own_ref, r_ref = refs[:3]
    s_ref, p_ref, x_ref, scal_ref = (None,) * 4 if first else refs[3:7]
    out_ref, ro_ref, so_ref, po_ref, xo_ref, scalo_ref = refs[-6:]
    faces = own_ref.shape[1]
    plan = Plan(width, faces)
    norm, alpha, beta = scalars(recv_ref[:, plan.half, :], faces, scal_ref)
    own = own_ref[...]
    p = own if first else own + beta * p_ref[...]
    po_ref[...] = p
    xo_ref[...] = alpha * p if first else x_ref[...] + alpha * p
    halves = []
    for n, w in enumerate(plan.owned(recv_ref)):
        s = w if first else w + beta * s_ref[n]
        so_ref[n] = s
        halves.append(r_ref[n] - alpha * s)
        ro_ref[n] = halves[n]
    plan.spread(out_ref, halves)
    scalo_ref[0:1, :] = jnp.broadcast_to(norm, (1, faces))
    scalo_ref[1:2, :] = jnp.broadcast_to(alpha, (1, faces))


def finish_kernel(width, recv_ref, own_ref, past_ref, p_ref, x_ref, scal_ref, xo_ref, ro_ref):
    faces = own_ref.shape[1]
    plan = Plan(width, faces)
    _, alpha, beta = scalars(recv_ref[:, width, :], faces, scal_ref)
    w = None
    for t in range(3):
        for q in range(plan.n_grp):
            piece = recv_ref[plan.base(t - 1, False) + q, :width, :]
            w = piece if w is None else w + piece
    own = own_ref[...]
    before = (past_ref[...] - own) / scal_ref[1:2, 0:1]
    xo_ref[...] = x_ref[...] + alpha * (own + beta * p_ref[...])
    ro_ref[...] = own - alpha * (w + beta * before)


def call(kernel, outs, args, scratch=(), name=None, space=pltpu.VMEM):
    vmem = pl.BlockSpec(memory_space=pltpu.VMEM)
    return pl.pallas_call(
        kernel,
        out_shape=outs,
        in_specs=[pl.BlockSpec(memory_space=space)] * len(args),
        out_specs=jax.tree.map(lambda _: vmem, outs),
        scratch_shapes=list(scratch),
        name=name,
        compiler_params=pltpu.CompilerParams(vmem_limit_bytes=VMEM_GRANT),
    )(*args)


def on_device(
    element_faces, interior_load, inverses, lift_operator, face_area, columns, blocks, diagonal
):
    n_dom, n_grp = lax.axis_size("dom"), lax.axis_size("grp")
    slots, width, full, faces = blocks.shape
    if width % 2 == 0 or n_dom < 6:
        raise ValueError("unsupported split")
    tall = up(full, 16)
    f32 = jnp.float32
    plan = Plan(width, faces)
    pieces = jax.ShapeDtypeStruct((n_dom * n_grp, plan.tall, faces), f32)
    wide_pieces = jax.ShapeDtypeStruct((n_dom * n_grp, up(width + 1, SUB), faces), f32)
    field = jax.ShapeDtypeStruct((width, faces), f32)
    halves = jax.ShapeDtypeStruct((2, plan.rows, faces), f32)

    def exchange(v):
        return lax.all_to_all(v, ALL, 0, 0)

    slab = pltpu.VMEM((tall, 3 * faces), f32)
    inputs = (columns, element_faces, inverses, interior_load, lift_operator, face_area)
    sent, hot, back, diag, held = call(
        functools.partial(rhs_kernel, width),
        (
            pieces,
            jax.ShapeDtypeStruct((3 * faces, slots * faces), jnp.bfloat16),
            jax.ShapeDtypeStruct((slots * faces, 3 * faces), jnp.bfloat16),
            field,
            jax.ShapeDtypeStruct(blocks.shape, f32),
        ),
        inputs + (diagonal, blocks),
        [pltpu.VMEM(a.shape, a.dtype) for a in inputs] + [slab, pltpu.SemaphoreType.DMA((len(inputs) + 2,))],
        name="rhs",
        space=pl.ANY,
    )
    sent, r = call(functools.partial(start_kernel, width), (pieces, halves), (exchange(sent),), name="start")
    past, state = None, ()
    for iteration in range(ITERS):
        first, last = iteration == 0, iteration + 1 == ITERS
        sent, own = call(
            functools.partial(apply_kernel, last),
            (wide_pieces if last else pieces, field),
            (exchange(sent), diag, held, hot, back),
            [slab, pltpu.VMEM((tall, slots * faces), f32), pltpu.VMEM((tall, slots * faces), f32)],
            name="apply",
        )
        got = exchange(sent)
        if last:
            _, p, x, scal = state
            return call(
                functools.partial(finish_kernel, width), (field, field), (got, own, past, p, x, scal), name="finish"
            )
        sent, r, *state = call(
            functools.partial(update_kernel, first, width),
            (pieces, halves, halves, field, field, jax.ShapeDtypeStruct((2, faces), f32)),
            (got, own, r) + tuple(state),
            name="update",
        )
        past = own


def solution(mesh):
    placed = (
        P(None, "dom"),
        P(None, "dom"),
        P("grp", None, "dom"),
        P("grp", None),
        P(None, "dom"),
        P(None, "dom"),
        P(None, "grp", None, "dom"),
        P("grp", "dom"),
    )
    return jax.shard_map(
        on_device,
        mesh=mesh,
        in_specs=placed,
        out_specs=(P("grp", "dom"), P("grp", "dom")),
        check_vma=False,
    )
```

```python
import functools

import jax
import jax.numpy as jnp
from jax import lax
from jax.experimental import pallas as pl
from jax.experimental.pallas import tpu as pltpu
from jax.sharding import PartitionSpec as P

ITERS = 8
SUB = 8
ALL = ("dom", "grp")
VMEM_GRANT = 16 * 1024 * 1024


def up(n, m):
    return (n + m - 1) // m * m


def parts3(x):
    hi = x.astype(jnp.bfloat16)
    rest = x - hi.astype(jnp.float32)
    mid = rest.astype(jnp.bfloat16)
    low = (rest - mid.astype(jnp.float32)).astype(jnp.bfloat16)
    return jnp.concatenate([hi, mid, low], axis=0)


def sum3(y):
    n = y.shape[0] // 3
    return y[:n] + y[n : 2 * n] + y[2 * n :]


class Plan:
    def __init__(self, width, faces):
        self.n_dom, self.n_grp = lax.axis_size("dom"), lax.axis_size("grp")
        self.width, self.faces = width, faces
        self.half = width // 2
        self.rows = self.half + 1
        self.tall = up(self.rows, SUB)

    def base(self, shift, lower):
        shift += self.n_dom // 2 if lower else 0
        return lax.rem(lax.axis_index("dom") + (shift + self.n_dom), self.n_dom) * self.n_grp

    def kept(self, shift):
        return self.base(shift - self.n_dom // 2, False)

    def left(self):
        return lax.broadcasted_iota(jnp.int32, (1, self.faces), 1) < self.faces // 2

    def split(self, rows, line):
        h, left = self.half, self.left()
        middle = rows[h : h + 1]
        upper = jnp.where(left, middle, line)
        lower = jnp.where(left, pltpu.roll(middle, self.faces // 2, 1), line)
        return (
            jnp.concatenate([rows[:h], upper], axis=0),
            jnp.concatenate([rows[h + 1 :], lower], axis=0),
        )

    def join(self, upper, lower):
        h = self.half
        middle = jnp.where(self.left(), upper[h : h + 1], pltpu.roll(lower[h : h + 1], self.faces // 2, 1))
        return jnp.concatenate([upper[:h], middle, lower[:h]], axis=0)

    def post(self, out_ref, slab_ref, line):
        w, f = self.width, self.faces
        for t in range(3):
            for q in range(self.n_grp):
                rows = slab_ref[q * w : (q + 1) * w, t * f : (t + 1) * f]
                for lower, piece in enumerate(self.split(rows, line)):
                    out_ref[self.base(t - 1, lower) + q, : self.rows, :] = piece

    def owned(self, recv_ref):
        sums = []
        for first in (functools.partial(self.base, lower=False), self.kept):
            total = None
            for t in range(3):
                for q in range(self.n_grp):
                    piece = recv_ref[first(t - 1) + q, : self.rows, :]
                    total = piece if total is None else total + piece
            row = lax.broadcasted_iota(jnp.int32, (self.rows, self.faces), 0)
            lane = lax.broadcasted_iota(jnp.int32, (self.rows, self.faces), 1)
            sums.append(jnp.where((row < self.half) | (lane < self.faces // 2), total, 0.0))
        return sums

    def spread(self, out_ref, halves):
        for first, piece in zip((functools.partial(self.base, lower=False), self.kept), halves):
            for t in range(3):
                for q in range(self.n_grp):
                    out_ref[first(t - 1) + q, : self.rows, :] = piece


def rhs_kernel(width, cols_hbm, owner_hbm, inv_hbm, load_hbm, lift_hbm, area_hbm, diag_hbm, blocks_hbm, out_ref, hot_ref, back_ref, diag_ref, blocks_ref, cols_ref, owner_ref, inv_ref, load_ref, lift_ref, area_ref, slab_ref, sems):
    fetches = [
        pltpu.make_async_copy(src, dst, sems.at[n])
        for n, (src, dst) in enumerate(
            (
                (cols_hbm, cols_ref), (owner_hbm, owner_ref), (load_hbm, load_ref), (inv_hbm, inv_ref),
                (lift_hbm, lift_ref), (area_hbm, area_ref), (diag_hbm, diag_ref), (blocks_hbm, blocks_ref),
            )
        )
    ]
    for fetch in fetches:
        fetch.start()
    faces = out_ref.shape[2]
    plan = Plan(width, faces)
    full = width * plan.n_grp
    slots, sides = cols_ref.shape[0], owner_ref.shape[0]
    low_face = (lax.axis_index("dom") - 1) * faces
    for fetch in fetches[:2]:
        fetch.wait()
    cols = cols_ref[...]
    here = jnp.where(cols >= 0, cols - low_face, -1)
    place = lax.broadcasted_iota(jnp.int32, (3 * faces, faces), 0)
    for s in range(slots):
        hit = place == here[s : s + 1, :]
        hot_ref[:, s * faces : (s + 1) * faces] = jnp.where(hit, 1.0, 0.0).astype(jnp.bfloat16)
    lists = jnp.concatenate([here, owner_ref[...] - low_face], axis=0)
    tall = up(slots + sides, SUB)
    blank = jnp.full((tall - slots - sides, faces), -1, jnp.int32)
    flipped = jnp.concatenate([lists, blank], axis=0).astype(jnp.float32).T
    window = lax.broadcasted_iota(jnp.int32, (faces, 3 * faces), 1).astype(jnp.float32)

    def scatter_of(n):
        return jnp.where(window == flipped[:, n : n + 1], 1.0, 0.0).astype(jnp.bfloat16)

    for s in range(slots):
        back_ref[s * faces : (s + 1) * faces, :] = scatter_of(s)
    for fetch in fetches[2:6]:
        fetch.wait()
    load = load_ref[...].astype(jnp.float32)
    rows = [
        jnp.sum(inv_ref[i].astype(jnp.float32) * load, axis=0, keepdims=True)
        for i in range(inv_ref.shape[0])
    ]
    u = jnp.concatenate(rows, axis=0)
    lifted = lax.dot_general(
        lift_ref[...], u, (((0,), (0,)), ((), ())),
        precision=lax.Precision.HIGHEST, preferred_element_type=jnp.float32,
    )
    pad = up(full, 16) - full
    total = None
    for k in range(sides):
        entry = -lifted[k * full : (k + 1) * full] * area_ref[k : k + 1, :]
        entry = jnp.concatenate([entry, jnp.zeros((pad, entry.shape[1]), jnp.float32)], axis=0)
        part = jnp.dot(parts3(entry), scatter_of(slots + k), preferred_element_type=jnp.float32)
        total = part if total is None else total + part
    slab_ref[...] = sum3(total)
    plan.post(out_ref, slab_ref, jnp.zeros((1, faces), jnp.float32))
    for fetch in fetches[6:]:
        fetch.wait()


def start_kernel(width, recv_ref, out_ref, r_ref):
    plan = Plan(width, recv_ref.shape[2])
    halves = plan.owned(recv_ref)
    plan.spread(out_ref, halves)
    r_ref[...] = jnp.stack(halves)


def apply_kernel(last, recv_ref, diag_ref, blocks_ref, hot_ref, back_ref, out_ref, own_ref, slab_ref, pick_ref, turn_ref):
    slots, width, full, faces = blocks_ref.shape
    plan = Plan(width, faces)
    n_dom, n_grp = plan.n_dom, plan.n_grp
    tall = slab_ref.shape[0]
    for t in range(3):
        for q in range(n_grp):
            rows = plan.join(*(recv_ref[plan.base(t - 1, lower) + q, : plan.rows, :] for lower in (False, True)))
            slab_ref[q * width : (q + 1) * width, t * faces : (t + 1) * faces] = rows
    me = lax.axis_index("grp")
    r = plan.join(*(recv_ref[plan.base(0, lower) + me, : plan.rows, :] for lower in (False, True)))
    own_ref[...] = r
    slab_ref[full:tall, :] = jnp.zeros((tall - full, 3 * faces), jnp.float32)
    wide = [jnp.broadcast_to(r[a : a + 1, :], (SUB, faces)) for a in range(width)]
    turn_ref[full:tall, :] = jnp.zeros((tall - full, slots * faces), jnp.float32)
    for low in range(0, full, SUB):
        high = min(low + SUB, full)
        for s in range(slots):
            turned = None
            for a in range(width):
                backward = blocks_ref[s, a, low:high, :] * wide[a][: high - low]
                turned = backward if turned is None else turned + backward
            turn_ref[low:high, s * faces : (s + 1) * faces] = turned
    pick_ref[...] = sum3(jnp.dot(parts3(slab_ref[...]), hot_ref[...], preferred_element_type=jnp.float32))
    slab_ref[...] = sum3(jnp.dot(parts3(turn_ref[...]), back_ref[...], preferred_element_type=jnp.float32))
    total = [None] * width
    for low in range(0, full, SUB):
        high = min(low + SUB, full)
        acc = [None] * width
        for s in range(slots):
            picked = pick_ref[low:high, s * faces : (s + 1) * faces]
            for a in range(width):
                forward = blocks_ref[s, a, low:high, :] * picked
                acc[a] = forward if acc[a] is None else acc[a] + forward
        for a in range(width):
            line = jnp.sum(acc[a], axis=0, keepdims=True)
            total[a] = line if total[a] is None else total[a] + line
    forward = jnp.concatenate(total, axis=0)
    plain = diag_ref[...] * r + forward
    square = jnp.sum(r * r, axis=0, keepdims=True)
    cross = jnp.sum(r * (plain + forward), axis=0, keepdims=True)
    fold = []
    for line in (square, cross):
        line = line + pltpu.roll(line, faces // 2, 1)
        fold.append(line + pltpu.roll(line, faces // 4, 1))
    lane = lax.broadcasted_iota(jnp.int32, (1, faces), 1)
    line = jnp.where(lane < faces // 4 * 3, fold[0], fold[1])
    if last:
        for n in range(n_dom * n_grp):
            out_ref[n, width : width + 1, :] = line
        for t in range(3):
            for q in range(n_grp):
                rows = slab_ref[q * width : (q + 1) * width, t * faces : (t + 1) * faces]
                out_ref[plan.base(t - 1, False) + q, :width, :] = rows
        mine = plan.base(0, False) + me
        out_ref[mine, :width, :] = out_ref[mine, :width, :] + plain
        return
    for n in range(n_dom * n_grp):
        out_ref[n, plan.half : plan.rows, :] = line
    plan.post(out_ref, slab_ref, line)
    for lower, piece in enumerate(plan.split(plain, jnp.zeros((1, faces), jnp.float32))):
        mine = plan.base(0, lower) + me
        out_ref[mine, : plan.rows, :] = out_ref[mine, : plan.rows, :] + piece


def scalars(lines, faces, scal_ref):
    lines = jnp.sum(lines, axis=0, keepdims=True)
    lane = lax.broadcasted_iota(jnp.int32, (1, faces), 1)
    norm_at = (lane >= faces // 2) & (lane < faces // 4 * 3)
    norm = jnp.sum(jnp.where(norm_at, lines, 0.0), axis=1, keepdims=True)
    cross = jnp.sum(jnp.where(lane >= faces // 4 * 3, lines, 0.0), axis=1, keepdims=True)
    if scal_ref is None:
        return norm, norm / cross, None
    beta = norm / scal_ref[0:1, 0:1]
    return norm, norm / (cross - beta * norm / scal_ref[1:2, 0:1]), beta


def update_kernel(first, width, *refs):
    recv_ref, own_ref, r_ref = refs[:3]
    s_ref, p_ref, x_ref, scal_ref = (None,) * 4 if first else refs[3:7]
    out_ref, ro_ref, so_ref, po_ref, xo_ref, scalo_ref = refs[-6:]
    faces = own_ref.shape[1]
    plan = Plan(width, faces)
    norm, alpha, beta = scalars(recv_ref[:, plan.half, :], faces, scal_ref)
    own = own_ref[...]
    p = own if first else own + beta * p_ref[...]
    po_ref[...] = p
    xo_ref[...] = alpha * p if first else x_ref[...] + alpha * p
    halves = []
    for n, w in enumerate(plan.owned(recv_ref)):
        s = w if first else w + beta * s_ref[n]
        so_ref[n] = s
        halves.append(r_ref[n] - alpha * s)
        ro_ref[n] = halves[n]
    plan.spread(out_ref, halves)
    scalo_ref[0:1, :] = jnp.broadcast_to(norm, (1, faces))
    scalo_ref[1:2, :] = jnp.broadcast_to(alpha, (1, faces))


def finish_kernel(width, recv_ref, own_ref, past_ref, p_ref, x_ref, scal_ref, xo_ref, ro_ref):
    faces = own_ref.shape[1]
    plan = Plan(width, faces)
    _, alpha, beta = scalars(recv_ref[:, width, :], faces, scal_ref)
    w = None
    for t in range(3):
        for q in range(plan.n_grp):
            piece = recv_ref[plan.base(t - 1, False) + q, :width, :]
            w = piece if w is None else w + piece
    own = own_ref[...]
    before = (past_ref[...] - own) / scal_ref[1:2, 0:1]
    xo_ref[...] = x_ref[...] + alpha * (own + beta * p_ref[...])
    ro_ref[...] = own - alpha * (w + beta * before)


def call(kernel, outs, args, scratch=(), name=None, space=pltpu.VMEM, grant=VMEM_GRANT):
    vmem = pl.BlockSpec(memory_space=pltpu.VMEM)
    return pl.pallas_call(
        kernel,
        out_shape=outs,
        in_specs=[pl.BlockSpec(memory_space=space)] * len(args),
        out_specs=jax.tree.map(lambda _: vmem, outs),
        scratch_shapes=list(scratch),
        name=name,
        compiler_params=pltpu.CompilerParams(vmem_limit_bytes=grant),
    )(*args)


def on_device(
    element_faces, interior_load, inverses, lift_operator, face_area, columns, blocks, diagonal
):
    n_dom, n_grp = lax.axis_size("dom"), lax.axis_size("grp")
    slots, width, full, faces = blocks.shape
    if width % 2 == 0 or n_dom < 6:
        raise ValueError("unsupported split")
    tall = up(full, 16)
    f32 = jnp.float32
    plan = Plan(width, faces)
    pieces = jax.ShapeDtypeStruct((n_dom * n_grp, plan.tall, faces), f32)
    wide_pieces = jax.ShapeDtypeStruct((n_dom * n_grp, up(width + 1, SUB), faces), f32)
    field = jax.ShapeDtypeStruct((width, faces), f32)
    halves = jax.ShapeDtypeStruct((2, plan.rows, faces), f32)

    def exchange(v):
        return lax.all_to_all(v, ALL, 0, 0)

    slab = pltpu.VMEM((tall, 3 * faces), f32)
    inputs = (columns, element_faces, inverses, interior_load, lift_operator, face_area)
    sent, hot, back, diag, held = call(
        functools.partial(rhs_kernel, width),
        (
            pieces,
            jax.ShapeDtypeStruct((3 * faces, slots * faces), jnp.bfloat16),
            jax.ShapeDtypeStruct((slots * faces, 3 * faces), jnp.bfloat16),
            field,
            jax.ShapeDtypeStruct(blocks.shape, f32),
        ),
        tuple(pltpu.with_memory_space_constraint(a, pltpu.HBM) for a in inputs + (diagonal, blocks)),
        [pltpu.VMEM(a.shape, a.dtype) for a in inputs] + [slab, pltpu.SemaphoreType.DMA((len(inputs) + 2,))],
        name="rhs",
        space=pl.ANY,
    )
    sent, r = call(functools.partial(start_kernel, width), (pieces, halves), (exchange(sent),), name="start")
    past, state = None, ()
    for iteration in range(ITERS):
        first, last = iteration == 0, iteration + 1 == ITERS
        sent, own = call(
            functools.partial(apply_kernel, last),
            (wide_pieces if last else pieces, field),
            (exchange(sent), diag, held, hot, back),
            [slab, pltpu.VMEM((tall, slots * faces), f32), pltpu.VMEM((tall, slots * faces), f32)],
            name="apply",
        )
        got = exchange(sent)
        if last:
            _, p, x, scal = state
            return call(
                functools.partial(finish_kernel, width), (field, field), (got, own, past, p, x, scal), name="finish"
            )
        sent, r, *state = call(
            functools.partial(update_kernel, first, width),
            (pieces, halves, halves, field, field, jax.ShapeDtypeStruct((2, faces), f32)),
            (got, own, r) + tuple(state),
            name="update",
        )
        past = own


def solution(mesh):
    placed = (
        P(None, "dom"),
        P(None, "dom"),
        P("grp", None, "dom"),
        P("grp", None),
        P(None, "dom"),
        P(None, "dom"),
        P(None, "grp", None, "dom"),
        P("grp", "dom"),
    )
    return jax.shard_map(
        on_device,
        mesh=mesh,
        in_specs=placed,
        out_specs=(P("grp", "dom"), P("grp", "dom")),
        check_vma=False,
    )
```

```python
import functools

import jax
import jax.numpy as jnp
from jax import lax
from jax.experimental import pallas as pl
from jax.experimental.pallas import tpu as pltpu
from jax.sharding import PartitionSpec as P

ITERS = 8
SUB = 8
ALL = ("dom", "grp")
VMEM_GRANT = 16 * 1024 * 1024
PARTS = 3


def up(n, m):
    return (n + m - 1) // m * m


def parts(x, count):
    out = [x.astype(jnp.bfloat16)]
    while len(out) < count:
        x = x - out[-1].astype(jnp.float32)
        out.append(x.astype(jnp.bfloat16))
    return jnp.concatenate(out, axis=0)


def whole(y, count):
    n = y.shape[0] // count
    return sum((y[k * n : (k + 1) * n] for k in range(1, count)), y[:n])


class Plan:
    def __init__(self, width, faces):
        self.n_dom, self.n_grp = lax.axis_size("dom"), lax.axis_size("grp")
        self.width, self.faces = width, faces
        self.half = width // 2
        self.rows = self.half + 1
        self.tall = up(self.rows, SUB)

    def base(self, shift, lower):
        shift += self.n_dom // 2 if lower else 0
        return lax.rem(lax.axis_index("dom") + (shift + self.n_dom), self.n_dom) * self.n_grp

    def kept(self, shift):
        return self.base(shift - self.n_dom // 2, False)

    def left(self):
        return lax.broadcasted_iota(jnp.int32, (1, self.faces), 1) < self.faces // 2

    def split(self, rows, line):
        h, left = self.half, self.left()
        middle = rows[h : h + 1]
        upper = jnp.where(left, middle, line)
        lower = jnp.where(left, pltpu.roll(middle, self.faces // 2, 1), line)
        return (
            jnp.concatenate([rows[:h], upper], axis=0),
            jnp.concatenate([rows[h + 1 :], lower], axis=0),
        )

    def join(self, upper, lower):
        h = self.half
        middle = jnp.where(self.left(), upper[h : h + 1], pltpu.roll(lower[h : h + 1], self.faces // 2, 1))
        return jnp.concatenate([upper[:h], middle, lower[:h]], axis=0)

    def post(self, out_ref, slab_ref, line):
        w, f = self.width, self.faces
        for t in range(3):
            for q in range(self.n_grp):
                rows = slab_ref[q * w : (q + 1) * w, t * f : (t + 1) * f]
                for lower, piece in enumerate(self.split(rows, line)):
                    out_ref[self.base(t - 1, lower) + q, : self.rows, :] = piece

    def owned(self, recv_ref):
        sums = []
        for first in (functools.partial(self.base, lower=False), self.kept):
            total = None
            for t in range(3):
                for q in range(self.n_grp):
                    piece = recv_ref[first(t - 1) + q, : self.rows, :]
                    total = piece if total is None else total + piece
            row = lax.broadcasted_iota(jnp.int32, (self.rows, self.faces), 0)
            lane = lax.broadcasted_iota(jnp.int32, (self.rows, self.faces), 1)
            sums.append(jnp.where((row < self.half) | (lane < self.faces // 2), total, 0.0))
        return sums

    def spread(self, out_ref, halves):
        for first, piece in zip((functools.partial(self.base, lower=False), self.kept), halves):
            for t in range(3):
                for q in range(self.n_grp):
                    out_ref[first(t - 1) + q, : self.rows, :] = piece


def rhs_kernel(width, cols_hbm, owner_hbm, inv_hbm, load_hbm, lift_hbm, area_hbm, diag_hbm, blocks_hbm, out_ref, hot_ref, back_ref, diag_ref, blocks_ref, cols_ref, owner_ref, inv_ref, load_ref, lift_ref, area_ref, slab_ref, sems):
    fetches = [
        pltpu.make_async_copy(src, dst, sems.at[n])
        for n, (src, dst) in enumerate(
            (
                (cols_hbm, cols_ref), (owner_hbm, owner_ref), (load_hbm, load_ref), (inv_hbm, inv_ref),
                (lift_hbm, lift_ref), (area_hbm, area_ref), (diag_hbm, diag_ref), (blocks_hbm, blocks_ref),
            )
        )
    ]
    for fetch in fetches:
        fetch.start()
    faces = out_ref.shape[2]
    plan = Plan(width, faces)
    full = width * plan.n_grp
    slots, sides = cols_ref.shape[0], owner_ref.shape[0]
    low_face = (lax.axis_index("dom") - 1) * faces
    for fetch in fetches[:2]:
        fetch.wait()
    cols = cols_ref[...]
    here = jnp.where(cols >= 0, cols - low_face, -1)
    place = lax.broadcasted_iota(jnp.int32, (3 * faces, faces), 0)
    for s in range(slots):
        hit = place == here[s : s + 1, :]
        hot_ref[:, s * faces : (s + 1) * faces] = jnp.where(hit, 1.0, 0.0).astype(jnp.bfloat16)
    lists = jnp.concatenate([here, owner_ref[...] - low_face], axis=0)
    tall = up(slots + sides, SUB)
    blank = jnp.full((tall - slots - sides, faces), -1, jnp.int32)
    flipped = jnp.concatenate([lists, blank], axis=0).astype(jnp.float32).T
    window = lax.broadcasted_iota(jnp.int32, (faces, 3 * faces), 1).astype(jnp.float32)

    def scatter_of(n):
        return jnp.where(window == flipped[:, n : n + 1], 1.0, 0.0).astype(jnp.bfloat16)

    for s in range(slots):
        back_ref[s * faces : (s + 1) * faces, :] = scatter_of(s)
    for fetch in fetches[2:6]:
        fetch.wait()
    load = load_ref[...].astype(jnp.float32)
    rows = [
        jnp.sum(inv_ref[i].astype(jnp.float32) * load, axis=0, keepdims=True)
        for i in range(inv_ref.shape[0])
    ]
    u = jnp.concatenate(rows, axis=0)
    lifted = lax.dot_general(
        lift_ref[...], u, (((0,), (0,)), ((), ())),
        precision=lax.Precision.HIGHEST, preferred_element_type=jnp.float32,
    )
    pad = up(full, 16) - full
    total = None
    for k in range(sides):
        entry = -lifted[k * full : (k + 1) * full] * area_ref[k : k + 1, :]
        entry = jnp.concatenate([entry, jnp.zeros((pad, entry.shape[1]), jnp.float32)], axis=0)
        part = jnp.dot(parts(entry, 3), scatter_of(slots + k), preferred_element_type=jnp.float32)
        total = part if total is None else total + part
    slab_ref[...] = whole(total, 3)
    plan.post(out_ref, slab_ref, jnp.zeros((1, faces), jnp.float32))
    for fetch in fetches[6:]:
        fetch.wait()


def start_kernel(width, recv_ref, out_ref, r_ref):
    plan = Plan(width, recv_ref.shape[2])
    halves = plan.owned(recv_ref)
    plan.spread(out_ref, halves)
    r_ref[...] = jnp.stack(halves)


def apply_kernel(last, recv_ref, diag_ref, blocks_ref, hot_ref, back_ref, out_ref, own_ref, slab_ref, pick_ref, turn_ref):
    slots, width, full, faces = blocks_ref.shape
    plan = Plan(width, faces)
    n_dom, n_grp = plan.n_dom, plan.n_grp
    tall = slab_ref.shape[0]
    for t in range(3):
        for q in range(n_grp):
            rows = plan.join(*(recv_ref[plan.base(t - 1, lower) + q, : plan.rows, :] for lower in (False, True)))
            slab_ref[q * width : (q + 1) * width, t * faces : (t + 1) * faces] = rows
    me = lax.axis_index("grp")
    r = plan.join(*(recv_ref[plan.base(0, lower) + me, : plan.rows, :] for lower in (False, True)))
    own_ref[...] = r
    slab_ref[full:tall, :] = jnp.zeros((tall - full, 3 * faces), jnp.float32)
    wide = [jnp.broadcast_to(r[a : a + 1, :], (SUB, faces)) for a in range(width)]
    turn_ref[full:tall, :] = jnp.zeros((tall - full, slots * faces), jnp.float32)
    window = parts(slab_ref[...], PARTS)
    groups = [slice(s * faces, min(s + 2, slots) * faces) for s in range(0, slots, 2)]

    def gather(at):
        picked = jnp.dot(window, hot_ref[:, at], preferred_element_type=jnp.float32)
        pick_ref[:, at] = whole(picked, PARTS)

    acc, rest, back = [None] * width, [None] * width, None
    gather(groups[0])
    for n, at in enumerate(groups):
        if n + 1 < len(groups):
            gather(groups[n + 1])
        for low in range(0, full, SUB):
            high = min(low + SUB, full)
            held = acc if high - low == SUB else rest
            for s in range(at.start // faces, at.stop // faces):
                cols = slice(s * faces, (s + 1) * faces)
                picked = pick_ref[low:high, cols]
                turned = None
                for a in range(width):
                    tile = blocks_ref[s, a, low:high, :]
                    forward = tile * picked
                    backward = tile * wide[a][: high - low]
                    held[a] = forward if held[a] is None else held[a] + forward
                    turned = backward if turned is None else turned + backward
                turn_ref[low:high, cols] = turned
        part = jnp.dot(parts(turn_ref[:, at], PARTS), back_ref[at, :], preferred_element_type=jnp.float32)
        back = part if back is None else back + part
    slab_ref[...] = whole(back, PARTS)
    lines = []
    for a in range(width):
        line = jnp.sum(acc[a], axis=0, keepdims=True)
        lines.append(line if rest[a] is None else line + jnp.sum(rest[a], axis=0, keepdims=True))
    forward = jnp.concatenate(lines, axis=0)
    plain = diag_ref[...] * r + forward
    square = jnp.sum(r * r, axis=0, keepdims=True)
    cross = jnp.sum(r * (plain + forward), axis=0, keepdims=True)
    fold = []
    for line in (square, cross):
        line = line + pltpu.roll(line, faces // 2, 1)
        fold.append(line + pltpu.roll(line, faces // 4, 1))
    lane = lax.broadcasted_iota(jnp.int32, (1, faces), 1)
    line = jnp.where(lane < faces // 4 * 3, fold[0], fold[1])
    if last:
        for n in range(n_dom * n_grp):
            out_ref[n, width : width + 1, :] = line
        for t in range(3):
            for q in range(n_grp):
                rows = slab_ref[q * width : (q + 1) * width, t * faces : (t + 1) * faces]
                out_ref[plan.base(t - 1, False) + q, :width, :] = rows
        mine = plan.base(0, False) + me
        out_ref[mine, :width, :] = out_ref[mine, :width, :] + plain
        return
    for n in range(n_dom * n_grp):
        out_ref[n, plan.half : plan.rows, :] = line
    plan.post(out_ref, slab_ref, line)
    for lower, piece in enumerate(plan.split(plain, jnp.zeros((1, faces), jnp.float32))):
        mine = plan.base(0, lower) + me
        out_ref[mine, : plan.rows, :] = out_ref[mine, : plan.rows, :] + piece


def scalars(lines, faces, scal_ref):
    lines = jnp.sum(lines, axis=0, keepdims=True)
    lane = lax.broadcasted_iota(jnp.int32, (1, faces), 1)
    norm_at = (lane >= faces // 2) & (lane < faces // 4 * 3)
    norm = jnp.sum(jnp.where(norm_at, lines, 0.0), axis=1, keepdims=True)
    cross = jnp.sum(jnp.where(lane >= faces // 4 * 3, lines, 0.0), axis=1, keepdims=True)
    if scal_ref is None:
        return norm, norm / cross, None
    beta = norm / scal_ref[0:1, 0:1]
    return norm, norm / (cross - beta * norm / scal_ref[1:2, 0:1]), beta


def update_kernel(first, width, *refs):
    recv_ref, own_ref, r_ref = refs[:3]
    s_ref, p_ref, x_ref, scal_ref = (None,) * 4 if first else refs[3:7]
    out_ref, ro_ref, so_ref, po_ref, xo_ref, scalo_ref = refs[-6:]
    faces = own_ref.shape[1]
    plan = Plan(width, faces)
    norm, alpha, beta = scalars(recv_ref[:, plan.half, :], faces, scal_ref)
    own = own_ref[...]
    p = own if first else own + beta * p_ref[...]
    po_ref[...] = p
    xo_ref[...] = alpha * p if first else x_ref[...] + alpha * p
    halves = []
    for n, w in enumerate(plan.owned(recv_ref)):
        s = w if first else w + beta * s_ref[n]
        so_ref[n] = s
        halves.append(r_ref[n] - alpha * s)
        ro_ref[n] = halves[n]
    plan.spread(out_ref, halves)
    scalo_ref[0:1, :] = jnp.broadcast_to(norm, (1, faces))
    scalo_ref[1:2, :] = jnp.broadcast_to(alpha, (1, faces))


def finish_kernel(width, recv_ref, own_ref, past_ref, p_ref, x_ref, scal_ref, xo_ref, ro_ref):
    faces = own_ref.shape[1]
    plan = Plan(width, faces)
    _, alpha, beta = scalars(recv_ref[:, width, :], faces, scal_ref)
    w = None
    for t in range(3):
        for q in range(plan.n_grp):
            piece = recv_ref[plan.base(t - 1, False) + q, :width, :]
            w = piece if w is None else w + piece
    own = own_ref[...]
    before = (past_ref[...] - own) / scal_ref[1:2, 0:1]
    xo_ref[...] = x_ref[...] + alpha * (own + beta * p_ref[...])
    ro_ref[...] = own - alpha * (w + beta * before)


def call(kernel, outs, args, scratch=(), name=None, space=pltpu.VMEM, grant=VMEM_GRANT):
    vmem = pl.BlockSpec(memory_space=pltpu.VMEM)
    return pl.pallas_call(
        kernel,
        out_shape=outs,
        in_specs=[pl.BlockSpec(memory_space=space)] * len(args),
        out_specs=jax.tree.map(lambda _: vmem, outs),
        scratch_shapes=list(scratch),
        name=name,
        compiler_params=pltpu.CompilerParams(vmem_limit_bytes=grant),
    )(*args)


def on_device(
    element_faces, interior_load, inverses, lift_operator, face_area, columns, blocks, diagonal
):
    n_dom, n_grp = lax.axis_size("dom"), lax.axis_size("grp")
    slots, width, full, faces = blocks.shape
    if width % 2 == 0 or n_dom < 6:
        raise ValueError("unsupported split")
    tall = up(full, 16)
    f32 = jnp.float32
    plan = Plan(width, faces)
    pieces = jax.ShapeDtypeStruct((n_dom * n_grp, plan.tall, faces), f32)
    wide_pieces = jax.ShapeDtypeStruct((n_dom * n_grp, up(width + 1, SUB), faces), f32)
    field = jax.ShapeDtypeStruct((width, faces), f32)
    halves = jax.ShapeDtypeStruct((2, plan.rows, faces), f32)

    def exchange(v):
        return lax.all_to_all(v, ALL, 0, 0)

    slab = pltpu.VMEM((tall, 3 * faces), f32)
    inputs = (columns, element_faces, inverses, interior_load, lift_operator, face_area)
    sent, hot, back, diag, held = call(
        functools.partial(rhs_kernel, width),
        (
            pieces,
            jax.ShapeDtypeStruct((3 * faces, slots * faces), jnp.bfloat16),
            jax.ShapeDtypeStruct((slots * faces, 3 * faces), jnp.bfloat16),
            field,
            jax.ShapeDtypeStruct(blocks.shape, f32),
        ),
        tuple(pltpu.with_memory_space_constraint(a, pltpu.HBM) for a in inputs + (diagonal, blocks)),
        [pltpu.VMEM(a.shape, a.dtype) for a in inputs] + [slab, pltpu.SemaphoreType.DMA((len(inputs) + 2,))],
        name="rhs",
        space=pl.ANY,
    )
    sent, r = call(functools.partial(start_kernel, width), (pieces, halves), (exchange(sent),), name="start")
    past, state = None, ()
    for iteration in range(ITERS):
        first, last = iteration == 0, iteration + 1 == ITERS
        sent, own = call(
            functools.partial(apply_kernel, last),
            (wide_pieces if last else pieces, field),
            (exchange(sent), diag, held, hot, back),
            [slab, pltpu.VMEM((tall, slots * faces), f32), pltpu.VMEM((tall, slots * faces), f32)],
            name="apply",
        )
        got = exchange(sent)
        if last:
            _, p, x, scal = state
            return call(
                functools.partial(finish_kernel, width), (field, field), (got, own, past, p, x, scal), name="finish"
            )
        sent, r, *state = call(
            functools.partial(update_kernel, first, width),
            (pieces, halves, halves, field, field, jax.ShapeDtypeStruct((2, faces), f32)),
            (got, own, r) + tuple(state),
            name="update",
        )
        past = own


def solution(mesh):
    placed = (
        P(None, "dom"),
        P(None, "dom"),
        P("grp", None, "dom"),
        P("grp", None),
        P(None, "dom"),
        P(None, "dom"),
        P(None, "grp", None, "dom"),
        P("grp", "dom"),
    )
    return jax.shard_map(
        on_device,
        mesh=mesh,
        in_specs=placed,
        out_specs=(P("grp", "dom"), P("grp", "dom")),
        check_vma=False,
    )
```

```python
import functools

import jax
import jax.numpy as jnp
from jax import lax
from jax.experimental import pallas as pl
from jax.experimental.pallas import tpu as pltpu
from jax.sharding import PartitionSpec as P

ITERS = 8
SUB = 8
ALL = ("dom", "grp")
VMEM_GRANT = 16 * 1024 * 1024
PARTS = 3


def up(n, m):
    return (n + m - 1) // m * m


def parts(x, count):
    out = [x.astype(jnp.bfloat16)]
    while len(out) < count:
        x = x - out[-1].astype(jnp.float32)
        out.append(x.astype(jnp.bfloat16))
    return jnp.concatenate(out, axis=0)


def whole(y, count):
    n = y.shape[0] // count
    return sum((y[k * n : (k + 1) * n] for k in range(1, count)), y[:n])


class Plan:
    def __init__(self, width, faces):
        self.n_dom, self.n_grp = lax.axis_size("dom"), lax.axis_size("grp")
        self.width, self.faces = width, faces
        self.step = faces // SUB
        self.dom = lax.axis_index("dom")
        self.lane = lax.broadcasted_iota(jnp.int32, (2, faces), 1)
        self.row = lax.broadcasted_iota(jnp.int32, (2, faces), 0)

    def wrap(self, n):
        return lax.rem(n + self.n_dom, self.n_dom)

    def owners(self, t):
        return lax.div(self.wrap(self.dom + (t - 1)), SUB) * (SUB * self.n_grp)

    def first(self):
        return lax.div(self.dom, SUB) * SUB

    def peer(self, i, t):
        return self.wrap(self.first() + (i + 1 - t)) * self.n_grp

    def free(self, j):
        cut = self.faces - self.step * j
        return (self.row == 1) & (self.lane >= cut - self.step) & (self.lane < cut)

    def post(self, out_ref, rows_of, line):
        for t in range(3):
            base = self.owners(t)
            for q in range(self.n_grp):
                rows = rows_of(t, q)
                rows = jnp.concatenate([rows, jnp.zeros((2 * SUB - self.width, self.faces), jnp.float32)], axis=0)
                for j in range(SUB):
                    share = rows[2 * j : 2 * j + 2]
                    if j:
                        share = jnp.where(self.lane < self.faces - self.step * j, share, rows[2 * j - 1 : 2 * j + 1])
                    if line is not None and t == 0:
                        share = jnp.where(self.free(j), line, share)
                    out_ref[base + (j * self.n_grp + q), t] = share

    def join(self, recv_ref, t, q):
        base = self.owners(t)
        shares = [recv_ref[base + j * self.n_grp + q, t] for j in range(SUB)]
        rows = []
        for j, share in enumerate(shares):
            below = shares[j + 1][0:1] if j + 1 < SUB else share[1:2]
            shifted = jnp.concatenate([share[1:2], below], axis=0)
            cut = self.faces - self.step * j
            rows.append(jnp.where(self.lane < cut - self.step * self.row, share, shifted))
        return jnp.concatenate(rows, axis=0)[: self.width]

    def owned(self, recv_ref):
        clear = self.free(lax.rem(self.dom, SUB))
        sums = []
        for i in range(SUB):
            total = None
            for t in range(3):
                for q in range(self.n_grp):
                    piece = recv_ref[self.peer(i, t) + q, t]
                    total = piece if total is None else total + piece
            sums.append(jnp.where(clear, 0.0, total))
        return sums

    def spread(self, out_ref, shares):
        for i, share in enumerate(shares):
            for t in range(3):
                for q in range(self.n_grp):
                    out_ref[self.peer(i, t) + q, t] = share


def rhs_kernel(width, cols_hbm, owner_hbm, inv_hbm, load_hbm, lift_hbm, area_hbm, diag_hbm, blocks_hbm, out_ref, hot_ref, back_ref, diag_ref, blocks_ref, cols_ref, owner_ref, inv_ref, load_ref, lift_ref, area_ref, slab_ref, sems):
    fetches = [
        pltpu.make_async_copy(src, dst, sems.at[n])
        for n, (src, dst) in enumerate(
            (
                (cols_hbm, cols_ref), (owner_hbm, owner_ref), (load_hbm, load_ref), (inv_hbm, inv_ref),
                (lift_hbm, lift_ref), (area_hbm, area_ref), (diag_hbm, diag_ref), (blocks_hbm, blocks_ref),
            )
        )
    ]
    for fetch in fetches:
        fetch.start()
    faces = out_ref.shape[-1]
    plan = Plan(width, faces)
    full = width * plan.n_grp
    slots, sides = cols_ref.shape[0], owner_ref.shape[0]
    low_face = (lax.axis_index("dom") - 1) * faces
    for fetch in fetches[:2]:
        fetch.wait()
    cols = cols_ref[...]
    here = jnp.where(cols >= 0, cols - low_face, -1)
    place = lax.broadcasted_iota(jnp.int32, (3 * faces, faces), 0)
    for s in range(slots):
        hit = place == here[s : s + 1, :]
        hot_ref[:, s * faces : (s + 1) * faces] = jnp.where(hit, 1.0, 0.0).astype(jnp.bfloat16)
    lists = jnp.concatenate([here, owner_ref[...] - low_face], axis=0)
    tall = up(slots + sides, SUB)
    blank = jnp.full((tall - slots - sides, faces), -1, jnp.int32)
    flipped = jnp.concatenate([lists, blank], axis=0).astype(jnp.float32).T
    window = lax.broadcasted_iota(jnp.int32, (faces, 3 * faces), 1).astype(jnp.float32)

    def scatter_of(n):
        return jnp.where(window == flipped[:, n : n + 1], 1.0, 0.0).astype(jnp.bfloat16)

    for s in range(slots):
        back_ref[s * faces : (s + 1) * faces, :] = scatter_of(s)
    for fetch in fetches[2:6]:
        fetch.wait()
    load = load_ref[...].astype(jnp.float32)
    rows = [
        jnp.sum(inv_ref[i].astype(jnp.float32) * load, axis=0, keepdims=True)
        for i in range(inv_ref.shape[0])
    ]
    u = jnp.concatenate(rows, axis=0)
    lifted = lax.dot_general(
        lift_ref[...], u, (((0,), (0,)), ((), ())),
        precision=lax.Precision.HIGHEST, preferred_element_type=jnp.float32,
    )
    pad = up(full, 16) - full
    total = None
    for k in range(sides):
        entry = -lifted[k * full : (k + 1) * full] * area_ref[k : k + 1, :]
        entry = jnp.concatenate([entry, jnp.zeros((pad, entry.shape[1]), jnp.float32)], axis=0)
        part = jnp.dot(parts(entry, 3), scatter_of(slots + k), preferred_element_type=jnp.float32)
        total = part if total is None else total + part
    slab_ref[...] = whole(total, 3)
    plan.post(out_ref, lambda t, q: slab_ref[q * width : (q + 1) * width, t * faces : (t + 1) * faces], None)
    for fetch in fetches[6:]:
        fetch.wait()


def start_kernel(width, recv_ref, out_ref, r_ref):
    plan = Plan(width, recv_ref.shape[-1])
    shares = plan.owned(recv_ref)
    plan.spread(out_ref, shares)
    for i, share in enumerate(shares):
        r_ref[i] = share


def apply_kernel(last, recv_ref, diag_ref, blocks_ref, hot_ref, back_ref, out_ref, own_ref, slab_ref, pick_ref, turn_ref):
    slots, width, full, faces = blocks_ref.shape
    plan = Plan(width, faces)
    n_dom, n_grp = plan.n_dom, plan.n_grp
    tall = slab_ref.shape[0]
    for t in range(3):
        for q in range(n_grp):
            slab_ref[q * width : (q + 1) * width, t * faces : (t + 1) * faces] = plan.join(recv_ref, t, q)
    me = lax.axis_index("grp")
    r = plan.join(recv_ref, 1, me)
    own_ref[...] = r
    slab_ref[full:tall, :] = jnp.zeros((tall - full, 3 * faces), jnp.float32)
    wide = [jnp.broadcast_to(r[a : a + 1, :], (SUB, faces)) for a in range(width)]
    turn_ref[full:tall, :] = jnp.zeros((tall - full, slots * faces), jnp.float32)
    window = parts(slab_ref[...], PARTS)
    groups = [slice(s * faces, min(s + 2, slots) * faces) for s in range(0, slots, 2)]

    def gather(at):
        picked = jnp.dot(window, hot_ref[:, at], preferred_element_type=jnp.float32)
        pick_ref[:, at] = whole(picked, PARTS)

    acc, rest, back = [None] * width, [None] * width, None
    gather(groups[0])
    for n, at in enumerate(groups):
        if n + 1 < len(groups):
            gather(groups[n + 1])
        for low in range(0, full, SUB):
            high = min(low + SUB, full)
            held = acc if high - low == SUB else rest
            for s in range(at.start // faces, at.stop // faces):
                cols = slice(s * faces, (s + 1) * faces)
                picked = pick_ref[low:high, cols]
                turned = None
                for a in range(width):
                    tile = blocks_ref[s, a, low:high, :]
                    forward = tile * picked
                    backward = tile * wide[a][: high - low]
                    held[a] = forward if held[a] is None else held[a] + forward
                    turned = backward if turned is None else turned + backward
                turn_ref[low:high, cols] = turned
        part = jnp.dot(parts(turn_ref[:, at], PARTS), back_ref[at, :], preferred_element_type=jnp.float32)
        back = part if back is None else back + part
    slab_ref[...] = whole(back, PARTS)
    lines = []
    for a in range(width):
        line = jnp.sum(acc[a], axis=0, keepdims=True)
        lines.append(line if rest[a] is None else line + jnp.sum(rest[a], axis=0, keepdims=True))
    forward = jnp.concatenate(lines, axis=0)
    plain = diag_ref[...] * r + forward
    square = jnp.sum(r * r, axis=0, keepdims=True)
    cross = jnp.sum(r * (plain + forward), axis=0, keepdims=True)
    fold = []
    for line in (square, cross):
        shift = faces // 2
        while shift * 2 >= plan.step:
            line = line + pltpu.roll(line, shift, 1)
            shift //= 2
        fold.append(line)
    lane = lax.broadcasted_iota(jnp.int32, (1, faces), 1)
    line = jnp.where(lax.rem(lane, plan.step) < plan.step // 2, fold[0], fold[1])

    def rows_of(t, q):
        rows = slab_ref[q * width : (q + 1) * width, t * faces : (t + 1) * faces]
        return rows + jnp.where(me == q, plain, 0.0) if t == 1 else rows

    if last:
        for n in range(n_dom * n_grp):
            out_ref[n, width : width + 1, :] = line
        for t in range(3):
            base = plan.wrap(plan.dom + (t - 1)) * n_grp
            for q in range(n_grp):
                out_ref[base + q, :width, :] = rows_of(t, q)
        return
    if n_dom > SUB:
        for n in range(n_dom * n_grp):
            out_ref[n, 0] = jnp.broadcast_to(line, (2, faces))
    plan.post(out_ref, rows_of, line)


def scalars(lines, start, step, scal_ref):
    line = jnp.sum(lines, axis=0, keepdims=True)
    lane = lax.broadcasted_iota(jnp.int32, line.shape, 1)
    middle = start + step // 2
    norm = jnp.sum(jnp.where((lane >= start) & (lane < middle), line, 0.0), axis=1, keepdims=True)
    cross = jnp.sum(jnp.where((lane >= middle) & (lane < start + step), line, 0.0), axis=1, keepdims=True)
    if scal_ref is None:
        return norm, norm / cross, None
    beta = norm / scal_ref[0:1, 0:1]
    return norm, norm / (cross - beta * norm / scal_ref[1:2, 0:1]), beta


def update_kernel(first, width, *refs):
    recv_ref, own_ref, r_ref = refs[:3]
    s_ref, p_ref, x_ref, scal_ref = (None,) * 4 if first else refs[3:7]
    out_ref, ro_ref, so_ref, po_ref, xo_ref, scalo_ref = refs[-6:]
    faces = own_ref.shape[1]
    plan = Plan(width, faces)
    start = faces - plan.step * (lax.rem(plan.dom, SUB) + 1)
    norm, alpha, beta = scalars(recv_ref[:, 0, 1, :], start, plan.step, scal_ref)
    shares = []
    for i, w in enumerate(plan.owned(recv_ref)):
        s = w if first else w + beta * s_ref[i]
        so_ref[i] = s
        shares.append(r_ref[i] - alpha * s)
        ro_ref[i] = shares[i]
    plan.spread(out_ref, shares)
    own = own_ref[...]
    p = own if first else own + beta * p_ref[...]
    po_ref[...] = p
    xo_ref[...] = alpha * p if first else x_ref[...] + alpha * p
    scalo_ref[0:1, :] = jnp.broadcast_to(norm, (1, faces))
    scalo_ref[1:2, :] = jnp.broadcast_to(alpha, (1, faces))


def finish_kernel(width, recv_ref, own_ref, past_ref, p_ref, x_ref, scal_ref, xo_ref, ro_ref):
    faces = own_ref.shape[1]
    plan = Plan(width, faces)
    _, alpha, beta = scalars(recv_ref[:, width, :], 0, plan.step, scal_ref)
    w = None
    for t in range(3):
        for q in range(plan.n_grp):
            piece = recv_ref[plan.wrap(plan.dom + (t - 1)) * plan.n_grp + q, :width, :]
            w = piece if w is None else w + piece
    own = own_ref[...]
    before = (past_ref[...] - own) / scal_ref[1:2, 0:1]
    xo_ref[...] = x_ref[...] + alpha * (own + beta * p_ref[...])
    ro_ref[...] = own - alpha * (w + beta * before)


def call(kernel, outs, args, scratch=(), name=None, space=pltpu.VMEM, grant=VMEM_GRANT):
    vmem = pl.BlockSpec(memory_space=pltpu.VMEM)
    return pl.pallas_call(
        kernel,
        out_shape=outs,
        in_specs=[pl.BlockSpec(memory_space=space)] * len(args),
        out_specs=jax.tree.map(lambda _: vmem, outs),
        scratch_shapes=list(scratch),
        name=name,
        compiler_params=pltpu.CompilerParams(vmem_limit_bytes=grant),
    )(*args)


def on_device(
    element_faces, interior_load, inverses, lift_operator, face_area, columns, blocks, diagonal
):
    n_dom, n_grp = lax.axis_size("dom"), lax.axis_size("grp")
    slots, width, full, faces = blocks.shape
    if width >= 2 * SUB or n_dom % SUB or faces % (16 * SUB):
        raise ValueError("unsupported split")
    tall = up(full, 16)
    f32 = jnp.float32
    pieces = jax.ShapeDtypeStruct((n_dom * n_grp, 3, 2, faces), f32)
    wide_pieces = jax.ShapeDtypeStruct((n_dom * n_grp, up(width + 1, SUB), faces), f32)
    field = jax.ShapeDtypeStruct((width, faces), f32)
    shares = jax.ShapeDtypeStruct((SUB, 2, faces), f32)

    def exchange(v):
        return lax.all_to_all(v, ALL, 0, 0)

    slab = pltpu.VMEM((tall, 3 * faces), f32)
    inputs = (columns, element_faces, inverses, interior_load, lift_operator, face_area)
    sent, hot, back, diag, held = call(
        functools.partial(rhs_kernel, width),
        (
            pieces,
            jax.ShapeDtypeStruct((3 * faces, slots * faces), jnp.bfloat16),
            jax.ShapeDtypeStruct((slots * faces, 3 * faces), jnp.bfloat16),
            field,
            jax.ShapeDtypeStruct(blocks.shape, f32),
        ),
        tuple(pltpu.with_memory_space_constraint(a, pltpu.HBM) for a in inputs + (diagonal, blocks)),
        [pltpu.VMEM(a.shape, a.dtype) for a in inputs] + [slab, pltpu.SemaphoreType.DMA((len(inputs) + 2,))],
        name="rhs",
        space=pl.ANY,
    )
    sent, r = call(functools.partial(start_kernel, width), (pieces, shares), (exchange(sent),), name="start")
    past, state = None, ()
    for iteration in range(ITERS):
        first, last = iteration == 0, iteration + 1 == ITERS
        sent, own = call(
            functools.partial(apply_kernel, last),
            (wide_pieces if last else pieces, field),
            (exchange(sent), diag, held, hot, back),
            [slab, pltpu.VMEM((tall, slots * faces), f32), pltpu.VMEM((tall, slots * faces), f32)],
            name="apply",
        )
        got = exchange(sent)
        if last:
            _, p, x, scal = state
            return call(
                functools.partial(finish_kernel, width), (field, field), (got, own, past, p, x, scal), name="finish"
            )
        sent, r, *state = call(
            functools.partial(update_kernel, first, width),
            (pieces, shares, shares, field, field, jax.ShapeDtypeStruct((2, faces), f32)),
            (got, own, r) + tuple(state),
            name="update",
        )
        past = own


def solution(mesh):
    placed = (
        P(None, "dom"),
        P(None, "dom"),
        P("grp", None, "dom"),
        P("grp", None),
        P(None, "dom"),
        P(None, "dom"),
        P(None, "grp", None, "dom"),
        P("grp", "dom"),
    )
    return jax.shard_map(
        on_device,
        mesh=mesh,
        in_specs=placed,
        out_specs=(P("grp", "dom"), P("grp", "dom")),
        check_vma=False,
    )
```

```python
import functools

import jax
import jax.numpy as jnp
from jax import lax
from jax.experimental import pallas as pl
from jax.experimental.pallas import tpu as pltpu
from jax.sharding import PartitionSpec as P

ITERS = 8
SUB = 8
ALL = ("dom", "grp")
VMEM_GRANT = 16 * 1024 * 1024
PARTS = 3


def up(n, m):
    return (n + m - 1) // m * m


def parts(x, count):
    out = [x.astype(jnp.bfloat16)]
    while len(out) < count:
        x = x - out[-1].astype(jnp.float32)
        out.append(x.astype(jnp.bfloat16))
    return jnp.concatenate(out, axis=0)


def whole(y, count):
    n = y.shape[0] // count
    return sum((y[k * n : (k + 1) * n] for k in range(1, count)), y[:n])


class Plan:
    def __init__(self, width, faces):
        self.n_dom, self.n_grp = lax.axis_size("dom"), lax.axis_size("grp")
        self.width, self.faces = width, faces
        self.step = faces // SUB
        self.dom = lax.axis_index("dom")
        self.lane = lax.broadcasted_iota(jnp.int32, (2, faces), 1)
        self.row = lax.broadcasted_iota(jnp.int32, (2, faces), 0)

    def wrap(self, n):
        return lax.rem(n + self.n_dom, self.n_dom)

    def owners(self, t):
        return lax.div(self.wrap(self.dom + (t - 1)), SUB) * (SUB * self.n_grp)

    def first(self):
        return lax.div(self.dom, SUB) * SUB

    def peer(self, i, t):
        return self.wrap(self.first() + (i + 1 - t)) * self.n_grp

    def free(self, j):
        cut = self.faces - self.step * j
        return (self.row == 1) & (self.lane >= cut - self.step) & (self.lane < cut)

    def post(self, out_ref, rows_of, line):
        for t in range(3):
            base = self.owners(t)
            for q in range(self.n_grp):
                rows = rows_of(t, q)
                rows = jnp.concatenate([rows, jnp.zeros((2 * SUB - self.width, self.faces), jnp.float32)], axis=0)
                for j in range(SUB):
                    share = rows[2 * j : 2 * j + 2]
                    if j:
                        share = jnp.where(self.lane < self.faces - self.step * j, share, rows[2 * j - 1 : 2 * j + 1])
                    if line is not None and t == 0:
                        share = jnp.where(self.free(j), line, share)
                    out_ref[base + (j * self.n_grp + q), t] = share

    def join(self, recv_ref, t, q):
        base = self.owners(t)
        shares = [recv_ref[base + j * self.n_grp + q, t] for j in range(SUB)]
        rows = []
        for j, share in enumerate(shares):
            below = shares[j + 1][0:1] if j + 1 < SUB else share[1:2]
            shifted = jnp.concatenate([share[1:2], below], axis=0)
            cut = self.faces - self.step * j
            rows.append(jnp.where(self.lane < cut - self.step * self.row, share, shifted))
        return jnp.concatenate(rows, axis=0)[: self.width]

    def owned(self, recv_ref):
        clear = self.free(lax.rem(self.dom, SUB))
        sums = []
        for i in range(SUB):
            total = None
            for t in range(3):
                for q in range(self.n_grp):
                    piece = recv_ref[self.peer(i, t) + q, t]
                    total = piece if total is None else total + piece
            sums.append(jnp.where(clear, 0.0, total))
        return sums

    def spread(self, out_ref, shares):
        for i, share in enumerate(shares):
            for t in range(3):
                for q in range(self.n_grp):
                    out_ref[self.peer(i, t) + q, t] = share


def rhs_kernel(width, cols_hbm, owner_hbm, inv_hbm, load_hbm, lift_hbm, area_hbm, diag_hbm, blocks_hbm, out_ref, hot_ref, back_ref, diag_ref, blocks_ref, cols_ref, owner_ref, inv_ref, load_ref, lift_ref, area_ref, slab_ref, sems):
    fetches = [
        pltpu.make_async_copy(src, dst, sems.at[n])
        for n, (src, dst) in enumerate(
            (
                (cols_hbm, cols_ref), (owner_hbm, owner_ref), (load_hbm, load_ref), (inv_hbm, inv_ref),
                (lift_hbm, lift_ref), (area_hbm, area_ref), (diag_hbm, diag_ref), (blocks_hbm, blocks_ref),
            )
        )
    ]
    for fetch in fetches:
        fetch.start()
    faces = out_ref.shape[-1]
    plan = Plan(width, faces)
    full = width * plan.n_grp
    slots, sides = cols_ref.shape[0], owner_ref.shape[0]
    low_face = (lax.axis_index("dom") - 1) * faces
    for fetch in fetches[:2]:
        fetch.wait()
    cols = cols_ref[...]
    here = jnp.where(cols >= 0, cols - low_face, -1)
    place = lax.broadcasted_iota(jnp.int32, (3 * faces, faces), 0)
    for s in range(slots):
        hit = place == here[s : s + 1, :]
        hot_ref[:, s * faces : (s + 1) * faces] = jnp.where(hit, 1.0, 0.0).astype(jnp.bfloat16)
    lists = jnp.concatenate([here, owner_ref[...] - low_face], axis=0)
    tall = up(slots + sides, SUB)
    blank = jnp.full((tall - slots - sides, faces), -1, jnp.int32)
    flipped = jnp.concatenate([lists, blank], axis=0).astype(jnp.float32).T
    window = lax.broadcasted_iota(jnp.int32, (faces, 3 * faces), 1).astype(jnp.float32)

    def scatter_of(n):
        return jnp.where(window == flipped[:, n : n + 1], 1.0, 0.0).astype(jnp.bfloat16)

    for s in range(slots):
        back_ref[s * faces : (s + 1) * faces, :] = scatter_of(s)
    for fetch in fetches[2:6]:
        fetch.wait()
    load = load_ref[...].astype(jnp.float32)
    rows = [
        jnp.sum(inv_ref[i].astype(jnp.float32) * load, axis=0, keepdims=True)
        for i in range(inv_ref.shape[0])
    ]
    u = jnp.concatenate(rows, axis=0)
    lifted = lax.dot_general(
        lift_ref[...], u, (((0,), (0,)), ((), ())),
        precision=lax.Precision.HIGHEST, preferred_element_type=jnp.float32,
    )
    pad = up(full, 16) - full
    total = None
    for k in range(sides):
        entry = -lifted[k * full : (k + 1) * full] * area_ref[k : k + 1, :]
        entry = jnp.concatenate([entry, jnp.zeros((pad, entry.shape[1]), jnp.float32)], axis=0)
        part = jnp.dot(parts(entry, 3), scatter_of(slots + k), preferred_element_type=jnp.float32)
        total = part if total is None else total + part
    slab_ref[...] = whole(total, 3)
    plan.post(out_ref, lambda t, q: slab_ref[q * width : (q + 1) * width, t * faces : (t + 1) * faces], None)
    for fetch in fetches[6:]:
        fetch.wait()


def start_kernel(width, recv_ref, out_ref, r_ref):
    plan = Plan(width, recv_ref.shape[-1])
    shares = plan.owned(recv_ref)
    plan.spread(out_ref, shares)
    for i, share in enumerate(shares):
        r_ref[i] = share


def apply_kernel(last, recv_ref, diag_ref, blocks_ref, hot_ref, back_ref, out_ref, own_ref, slab_ref, pick_ref, turn_ref):
    slots, width, full, faces = blocks_ref.shape
    plan = Plan(width, faces)
    n_dom, n_grp = plan.n_dom, plan.n_grp
    tall = slab_ref.shape[0]
    for t in range(3):
        for q in range(n_grp):
            slab_ref[q * width : (q + 1) * width, t * faces : (t + 1) * faces] = plan.join(recv_ref, t, q)
    me = lax.axis_index("grp")
    r = plan.join(recv_ref, 1, me)
    own_ref[...] = r
    slab_ref[full:tall, :] = jnp.zeros((tall - full, 3 * faces), jnp.float32)
    wide = [jnp.broadcast_to(r[a : a + 1, :], (SUB, faces)) for a in range(width)]
    turn_ref[full:tall, :] = jnp.zeros((tall - full, slots * faces), jnp.float32)
    window = parts(slab_ref[...], PARTS)
    groups = [slice(s * faces, min(s + 2, slots) * faces) for s in range(0, slots, 2)]

    def gather(at):
        picked = jnp.dot(window, hot_ref[:, at], preferred_element_type=jnp.float32)
        pick_ref[:, at] = whole(picked, PARTS)

    acc, rest, back = [None] * width, [None] * width, None
    gather(groups[0])
    for n, at in enumerate(groups):
        if n + 1 < len(groups):
            gather(groups[n + 1])
        for low in range(0, full, SUB):
            high = min(low + SUB, full)
            held = acc if high - low == SUB else rest
            for s in range(at.start // faces, at.stop // faces):
                cols = slice(s * faces, (s + 1) * faces)
                picked = pick_ref[low:high, cols]
                turned = None
                for a in range(width):
                    tile = blocks_ref[s, a, low:high, :]
                    forward = tile * picked
                    backward = tile * wide[a][: high - low]
                    held[a] = forward if held[a] is None else held[a] + forward
                    turned = backward if turned is None else turned + backward
                turn_ref[low:high, cols] = turned
        part = jnp.dot(parts(turn_ref[:, at], PARTS), back_ref[at, :], preferred_element_type=jnp.float32)
        back = part if back is None else back + part
    slab_ref[...] = whole(back, PARTS)
    lines = []
    for a in range(width):
        line = jnp.sum(acc[a], axis=0, keepdims=True)
        lines.append(line if rest[a] is None else line + jnp.sum(rest[a], axis=0, keepdims=True))
    forward = jnp.concatenate(lines, axis=0)
    plain = diag_ref[...] * r + forward
    square = jnp.sum(r * r, axis=0, keepdims=True)
    cross = jnp.sum(r * (plain + forward), axis=0, keepdims=True)
    fold = []
    for line in (square, cross):
        shift = faces // 2
        while shift * 2 >= plan.step:
            line = line + pltpu.roll(line, shift, 1)
            shift //= 2
        fold.append(line)
    lane = lax.broadcasted_iota(jnp.int32, (1, faces), 1)
    line = jnp.where(lax.rem(lane, plan.step) < plan.step // 2, fold[0], fold[1])

    def rows_of(t, q):
        rows = slab_ref[q * width : (q + 1) * width, t * faces : (t + 1) * faces]
        return rows + jnp.where(me == q, plain, 0.0) if t == 1 else rows

    if last:
        for n in range(n_dom * n_grp):
            out_ref[n, width : width + 1, :] = line
        for t in range(3):
            base = plan.wrap(plan.dom + (t - 1)) * n_grp
            for q in range(n_grp):
                out_ref[base + q, :width, :] = rows_of(t, q)
        return
    if n_dom > SUB:
        for n in range(n_dom * n_grp):
            out_ref[n, 0] = jnp.broadcast_to(line, (2, faces))
    plan.post(out_ref, rows_of, line)


def scalars(lines, start, step, scal_ref):
    line = jnp.sum(lines, axis=0, keepdims=True)
    lane = lax.broadcasted_iota(jnp.int32, line.shape, 1)
    middle = start + step // 2
    norm = jnp.sum(jnp.where((lane >= start) & (lane < middle), line, 0.0), axis=1, keepdims=True)
    cross = jnp.sum(jnp.where((lane >= middle) & (lane < start + step), line, 0.0), axis=1, keepdims=True)
    if scal_ref is None:
        return norm, norm / cross, None
    beta = norm / scal_ref[0:1, 0:1]
    return norm, norm / (cross - beta * norm / scal_ref[1:2, 0:1]), beta


def update_kernel(first, keep, width, *refs):
    recv_ref, own_ref, r_ref = refs[:3]
    p_ref, x_ref, scal_ref, s_ref = (None,) * 4 if first else refs[3:7]
    out_ref, po_ref, xo_ref, scalo_ref = refs[-(6 if keep else 4) :][:4]
    faces = own_ref.shape[1]
    plan = Plan(width, faces)
    start = faces - plan.step * (lax.rem(plan.dom, SUB) + 1)
    norm, alpha, beta = scalars(recv_ref[:, 0, 1, :], start, plan.step, scal_ref)
    shares = []
    for i, w in enumerate(plan.owned(recv_ref)):
        s = w if first else w + beta * s_ref[i]
        shares.append(r_ref[i] - alpha * s)
        if keep:
            ro_ref, so_ref = refs[-2:]
            ro_ref[i] = shares[i]
            so_ref[i] = s
    plan.spread(out_ref, shares)
    own = own_ref[...]
    p = own if first else own + beta * p_ref[...]
    po_ref[...] = p
    xo_ref[...] = alpha * p if first else x_ref[...] + alpha * p
    scalo_ref[0:1, :] = jnp.broadcast_to(norm, (1, faces))
    scalo_ref[1:2, :] = jnp.broadcast_to(alpha, (1, faces))


def finish_kernel(width, recv_ref, own_ref, past_ref, p_ref, x_ref, scal_ref, xo_ref, ro_ref):
    faces = own_ref.shape[1]
    plan = Plan(width, faces)
    _, alpha, beta = scalars(recv_ref[:, width, :], 0, plan.step, scal_ref)
    w = None
    for t in range(3):
        for q in range(plan.n_grp):
            piece = recv_ref[plan.wrap(plan.dom + (t - 1)) * plan.n_grp + q, :width, :]
            w = piece if w is None else w + piece
    own = own_ref[...]
    before = (past_ref[...] - own) / scal_ref[1:2, 0:1]
    xo_ref[...] = x_ref[...] + alpha * (own + beta * p_ref[...])
    ro_ref[...] = own - alpha * (w + beta * before)


def call(kernel, outs, args, scratch=(), name=None, space=pltpu.VMEM):
    vmem = pl.BlockSpec(memory_space=pltpu.VMEM)
    return pl.pallas_call(
        kernel,
        out_shape=outs,
        in_specs=[pl.BlockSpec(memory_space=space)] * len(args),
        out_specs=jax.tree.map(lambda _: vmem, outs),
        scratch_shapes=list(scratch),
        name=name,
        compiler_params=pltpu.CompilerParams(vmem_limit_bytes=VMEM_GRANT),
    )(*args)


def on_device(
    element_faces, interior_load, inverses, lift_operator, face_area, columns, blocks, diagonal
):
    n_dom, n_grp = lax.axis_size("dom"), lax.axis_size("grp")
    slots, width, full, faces = blocks.shape
    if width >= 2 * SUB or n_dom % SUB or faces % (16 * SUB):
        raise ValueError("unsupported split")
    tall = up(full, 16)
    f32 = jnp.float32
    pieces = jax.ShapeDtypeStruct((n_dom * n_grp, 3, 2, faces), f32)
    wide_pieces = jax.ShapeDtypeStruct((n_dom * n_grp, up(width + 1, SUB), faces), f32)
    field = jax.ShapeDtypeStruct((width, faces), f32)
    shares = jax.ShapeDtypeStruct((SUB, 2, faces), f32)

    def exchange(v):
        return lax.all_to_all(v, ALL, 0, 0)

    slab = pltpu.VMEM((tall, 3 * faces), f32)
    inputs = (columns, element_faces, inverses, interior_load, lift_operator, face_area)
    sent, hot, back, diag, held = call(
        functools.partial(rhs_kernel, width),
        (
            pieces,
            jax.ShapeDtypeStruct((3 * faces, slots * faces), jnp.bfloat16),
            jax.ShapeDtypeStruct((slots * faces, 3 * faces), jnp.bfloat16),
            field,
            jax.ShapeDtypeStruct(blocks.shape, f32),
        ),
        tuple(pltpu.with_memory_space_constraint(a, pltpu.HBM) for a in inputs + (diagonal, blocks)),
        [pltpu.VMEM(a.shape, a.dtype) for a in inputs] + [slab, pltpu.SemaphoreType.DMA((len(inputs) + 2,))],
        name="rhs",
        space=pl.ANY,
    )
    sent, r = call(functools.partial(start_kernel, width), (pieces, shares), (exchange(sent),), name="start")
    past, state = None, ()
    for iteration in range(ITERS):
        first, last = iteration == 0, iteration + 1 == ITERS
        sent, own = call(
            functools.partial(apply_kernel, last),
            (wide_pieces if last else pieces, field),
            (exchange(sent), diag, held, hot, back),
            [slab, pltpu.VMEM((tall, slots * faces), f32), pltpu.VMEM((tall, slots * faces), f32)],
            name="apply",
        )
        got = exchange(sent)
        if last:
            p, x, scal = state
            return call(
                functools.partial(finish_kernel, width), (field, field), (got, own, past, p, x, scal), name="finish"
            )
        keep = iteration + 2 < ITERS
        sent, *state = call(
            functools.partial(update_kernel, first, keep, width),
            (pieces, field, field, jax.ShapeDtypeStruct((2, faces), f32)) + ((shares, shares) if keep else ()),
            (got, own, r) + tuple(state) + (() if first else (s,)),
            name="update",
        )
        if keep:
            *state, r, s = state
        past = own


def solution(mesh):
    placed = (
        P(None, "dom"),
        P(None, "dom"),
        P("grp", None, "dom"),
        P("grp", None),
        P(None, "dom"),
        P(None, "dom"),
        P(None, "grp", None, "dom"),
        P("grp", "dom"),
    )
    return jax.shard_map(
        on_device,
        mesh=mesh,
        in_specs=placed,
        out_specs=(P("grp", "dom"), P("grp", "dom")),
        check_vma=False,
    )
```
